256 devices in a mesh: tm: 32 (over z, y), coef: 8 (over x, core).
Axes of the slice: x: 4, y: 4, z: 8, core: 2. Of those that a mesh axis runs over, the one named last changes fastest.
Arguments:
- design: bfloat16 [8192, 50176], P('tm', 'coef'), may hold values from -0.0546875 to 0.0546875
- observed: float32 [8192, 128], P('tm'), may hold values from -6 to 6
- slab_counts: int32 [32], P('tm'), may hold values from 128 to 256, as said below
- gap_mask: int32 [8192], P('tm'), may hold values 0 or 1
- filter_taps: float32 [128], replicated, may hold values from -0.5 to 1.2, as said below
- kaula_diag: float32 [50176], P('coef'), may hold values from 0.1 to 1
- precond: float32 [50176], P('coef'), may hold values from 0.3 to 3
Outputs:
- solution: float32 [50176, 128], P(('coef', 'tm'))
- residual: float32 [50176, 128], P(('coef', 'tm'))
The draws below stay inside these ranges and needn't reach their ends.
Inputs may be any that keep to these rules, and one draw needn't show every extreme that they name: `slab_counts`: every slab holds at most 256 valid epochs, and some slab holds exactly 256. filter_taps[0] lies between 1 and 1.2.
All inputs are finite; a program needn't handle non-finite values. No bound on the sum of `gap_mask` on one device may be relied on, other than what follows from the above.
Results may differ from the reference program's by a relative error of at most 0.0065.
The reference program's roundings to bfloat16 on the way (of `weighted`) count: a program that leaves them out, or rounds other values in their place, can miss the bound.
Values may be sent and summed in bfloat16 or wider, within the bound.
A program may use at most 64 MiB of HBM per device.

```python
import math
import jax
import jax.numpy as jnp
from jax import lax

NC = 50176
R = 128
E_DEV = 256
BAND = 128
ITERS = 2
EPOCHS = 8192
N_TM = 32


def draw_slab_counts(key, part):
    first_key = jax.random.fold_in(key, 11)
    second_key = jax.random.fold_in(key, 12)
    values = jax.random.randint(first_key, (N_TM,), E_DEV // 2, E_DEV + 1)
    chosen = jax.random.randint(second_key, (), 0, N_TM)
    return jnp.where(jnp.arange(N_TM) == chosen, E_DEV, values).astype(jnp.int32)


def draw_filter_taps(key, part):
    first_key = jax.random.fold_in(key, 21)
    second_key = jax.random.fold_in(key, 22)
    lags = jnp.arange(BAND).astype(jnp.float32)
    decay = jnp.exp(-1.5 * lags / BAND)
    noise = 0.12 * jnp.clip(jax.random.normal(first_key, (BAND,), jnp.float32), -4.0, 4.0)
    leading = 1.0 + 0.2 * jax.random.uniform(second_key, (BAND,), jnp.float32)
    return jnp.where(lags == 0.0, leading, decay * noise).astype(jnp.float32)


def plant(values, rng, smallest, high):
    place = [jax.random.randint(jax.random.fold_in(rng, axis), (), 0, length) for axis, length in enumerate(values.shape)]
    widest = values.shape.index(max(values.shape))
    next_to = place[:widest] + [(place[widest] + 1) % values.shape[widest]] + place[widest + 1:]
    return values.at[tuple(place)].set(smallest).at[tuple(next_to)].set(high)


def with_spikes(drawn, rng, source, target, parts, factor):
    def block_of(dim):
        return (jnp.arange(drawn.shape[dim]) // (drawn.shape[dim] // parts)).reshape((-1,) + (1,) * (drawn.ndim - 1 - dim))

    one_side = jax.random.permutation(rng, parts)[block_of(target)]
    second = (block_of(target) + parts // 2) % parts
    return jnp.where((block_of(source) == one_side) | (block_of(source) == second), factor * drawn, drawn)


def shard_levels(stream_key, extent, split, low, top_value):
    factor_of, own = 1.0, jax.random.fold_in(stream_key, 6)
    for axis_at, parts in split:
        heights = jnp.exp(jax.random.uniform(jax.random.fold_in(own, axis_at), (parts,), jnp.float32, low / len(split), top_value / len(split)))
        factor_of = factor_of * jnp.repeat(heights, extent[axis_at] // parts).reshape([-1 if axis == axis_at else 1 for axis in range(len(extent))])
    return factor_of


def centred(own_key, dims, scale, reach, pieces=(), kind=jnp.bfloat16):
    values = scale * jax.random.normal(own_key, dims, jnp.float32)
    if pieces:
        values = values * shard_levels(own_key, dims, pieces, -0.22, 0.18)
    return jnp.clip(values, -reach, reach).astype(kind)


def noise_with(rng, dims, scale, reach, split, heavy, held_as=jnp.bfloat16):
    values = scale * jax.random.normal(rng, dims, jnp.float32)
    if split:
        values = values * shard_levels(rng, dims, split, -0.22, 0.18)
    return jnp.clip(with_spikes(values, jax.random.fold_in(rng, 3), *heavy), -reach, reach).astype(held_as)


def setup_inputs(seed: int = 0) -> dict:
    key_list = jax.random.split(jax.random.key(seed), 8)
    return {
        "design": noise_with(key_list[0], (EPOCHS, NC), NC ** -0.5, 0.0546875, ((0, 32), (1, 8)), (0, 1, 32, 2.75)),
        "observed": centred(key_list[1], (EPOCHS, R), 1.0, 6.0, ((0, 32),), jnp.float32),
        "slab_counts": draw_slab_counts(jax.random.fold_in(key_list[7], 71), 0),
        "gap_mask": plant((jax.random.randint(key_list[3], (EPOCHS,), 0, 8) < 7).astype(jnp.int32), jax.random.fold_in(key_list[3], 1), 0, 1),
        "filter_taps": draw_filter_taps(jax.random.fold_in(key_list[7], 71), 0),
        "kaula_diag": jnp.clip(jnp.exp(math.log(1.0) - 2.3025851 * jax.random.uniform(key_list[5], (NC,), jnp.float32) ** shard_levels(key_list[5], (NC,), ((0, 8),), -0.2, 0.2)), 0.1, 1.0),
        "precond": jnp.clip(jnp.exp(math.log(3.0) - 2.3025851 * jax.random.uniform(key_list[6], (NC,), jnp.float32) ** shard_levels(key_list[6], (NC,), ((0, 8),), -0.2, 0.2)), 0.3, 3.0),
    }


def toeplitz(pattern, band_len):
    tiled = jnp.tile(pattern, band_len)[: band_len * (2 * band_len - 1)]
    return tiled.reshape(band_len, 2 * band_len - 1)[:, :band_len]


def block_pair(filter_taps):
    band_len = filter_taps.shape[0]
    spacer = jnp.zeros((band_len,), jnp.float32)
    reversed_taps = filter_taps[:0:-1]
    lower = jnp.concatenate([filter_taps[:1], spacer, reversed_taps])
    upper = jnp.concatenate([jnp.zeros((1,), jnp.float32), reversed_taps, spacer])
    return toeplitz(lower, band_len), toeplitz(upper, band_len)


def forward(values, lower_block, upper_block):
    band_len = lower_block.shape[0]
    blocks = values.reshape(-1, band_len, values.shape[1])
    previous = jnp.concatenate([jnp.zeros_like(blocks[:1]), blocks[:-1]], 0)
    result = jnp.einsum("ij,bjr->bir", lower_block, blocks, precision=lax.Precision.HIGHEST)
    result = result + jnp.einsum("ij,bjr->bir", upper_block, previous, precision=lax.Precision.HIGHEST)
    return result.reshape(values.shape)


def backward(values, lower_block, upper_block):
    band_len = lower_block.shape[0]
    blocks = values.reshape(-1, band_len, values.shape[1])
    following = jnp.concatenate([blocks[1:], jnp.zeros_like(blocks[:1])], 0)
    result = jnp.einsum("ji,bjr->bir", lower_block, blocks, precision=lax.Precision.HIGHEST)
    result = result + jnp.einsum("ji,bjr->bir", upper_block, following, precision=lax.Precision.HIGHEST)
    return result.reshape(values.shape)


def reference(design, observed, slab_counts, gap_mask, filter_taps, kaula_diag, precond):
    lower_block, upper_block = block_pair(filter_taps)
    position = jnp.arange(EPOCHS, dtype=jnp.int32)
    slab_index = position // E_DEV
    weight = ((gap_mask == 1) & (position % E_DEV < slab_counts[slab_index])).astype(jnp.float32)[:, None]

    def weighted(values):
        inner = forward(weight * values, lower_block, upper_block)
        return (weight * backward(inner, lower_block, upper_block)).astype(jnp.bfloat16)

    def transposed(filtered):
        return lax.dot_general(design, filtered, (((0,), (0,)), ((), ())), preferred_element_type=jnp.float32)

    kaula_col = kaula_diag[:, None]
    precond_col = precond[:, None]
    residual = transposed(weighted(observed))
    solution = jnp.zeros_like(residual)
    scaled = precond_col * residual
    direction = scaled
    norm_now = jnp.sum(residual * scaled, 0)
    for iteration in range(ITERS):
        slab_values = jnp.dot(design, direction.astype(jnp.bfloat16), preferred_element_type=jnp.float32)
        image = transposed(weighted(slab_values)) + kaula_col * direction
        step_len = norm_now / jnp.sum(direction * image, 0)
        solution = solution + step_len * direction
        residual = residual - step_len * image
        scaled = precond_col * residual
        norm_next = jnp.sum(residual * scaled, 0)
        direction = scaled + (norm_next / norm_now) * direction
        norm_now = norm_next
    return solution, residual
```

```python
import functools

import jax
import jax.numpy as jnp
from jax import lax
from jax.experimental import pallas as pl
from jax.experimental.pallas import tpu as pltpu
from jax.sharding import Mesh
from jax.sharding import PartitionSpec as P

AXES = ("z", "y", "x", "c")
TM = ("z", "y")
COEF = ("x", "c")
MESH = pl.DeviceIdType.MESH
NZ, NY, NX, NC = 8, 4, 4, 2
NA, NB = 104, 92
RA, RB = 112, 96
BAND = 128
F32 = jnp.float32
BF16 = jnp.bfloat16
HIGH = lax.Precision.HIGHEST


def dot(a, b, precision=None):
    return jnp.dot(a, b, preferred_element_type=F32, precision=precision)


def rcopy(src, dst, ssem, rsem, **device):
    return pltpu.make_async_remote_copy(
        src_ref=src, dst_ref=dst, send_sem=ssem, recv_sem=rsem, device_id=device, device_id_type=MESH
    )


def kernel(
    aa, ab, ata, atb, obs, wm, lo, up, lot, upt, kda, kdb, pca, pcb,
    xout, rout,
    bm, y_a, y_b,
    sa, ra, sya, rya, sb, rb, szb, rzb,
    ga, gb, vs, vr, us, ur, hx, scs, scr, scc,
    sem_sa, sem_ra, sem_sya, sem_rya, sem_sb, sem_rb, sem_szb, sem_rzb,
    sem_gs, sem_ga, sem_gay, sem_gb, sem_gby,
    sem_vs, sem_vr, sem_us, sem_ur, sem_hs, sem_hr, sem_cs, sem_cr,
):
    z, y, x, c = (lax.axis_index(name) for name in AXES)
    t = z * NY + y
    zp = [lax.rem(z + k, NZ) for k in range(NZ)]
    zm = [lax.rem(z + NZ - k, NZ) for k in range(NZ)]
    yp = [lax.rem(y + k, NY) for k in range(NY)]
    ym = [lax.rem(y + NY - k, NY) for k in range(NY)]
    xp = [lax.rem(x + k, NX) for k in range(NX)]
    other = 1 - c
    t_up = lax.rem(t + 1, NZ * NY)
    t_down = lax.rem(t + NZ * NY - 1, NZ * NY)
    pending = []

    def send(src, dst, ssem, rsem, **device):
        copy = rcopy(src, dst, ssem, rsem, **device)
        copy.start()
        pending.append(copy)

    def arrived(dst, ssem, rsem, **device):
        rcopy(dst, dst, ssem, rsem, **device).wait_recv()

    barrier = pltpu.get_barrier_semaphore()
    peers = [dict(z=zp[k]) for k in range(1, NZ)] + [dict(y=yp[k]) for k in range(1, NY)]
    peers += [dict(x=xp[k]) for k in range(1, NX)] + [dict(c=other)]
    for step in (t_up, t_down):
        for core in range(NC):
            peers.append(dict(z=lax.div(step, NY), y=lax.rem(step, NY), c=jnp.int32(core)))
    for peer in peers:
        pl.semaphore_signal(barrier, inc=1, device_id=peer, device_id_type=MESH)

    keep_first = jnp.where(t == 0, 0.0, 1.0).astype(F32)
    keep_last = jnp.where(t == NZ * NY - 1, 0.0, 1.0).astype(F32)
    ll = dot(lot[...], lo[...], HIGH)
    uu = dot(upt[...], up[...], HIGH)
    lu = dot(lot[...], up[...], HIGH)
    ul = dot(upt[...], lo[...], HIGH)
    zero = jnp.zeros((BAND, BAND), F32)
    bm[0:BAND, 0:BAND] = keep_first * lu
    bm[0:BAND, BAND : 2 * BAND] = ll + uu
    bm[0:BAND, 2 * BAND : 3 * BAND] = ul
    bm[0:BAND, 3 * BAND :] = zero
    bm[BAND:, 0:BAND] = zero
    bm[BAND:, BAND : 2 * BAND] = lu
    bm[BAND:, 2 * BAND : 3 * BAND] = ll + keep_last * uu
    bm[BAND:, 3 * BAND :] = keep_last * ul

    def filtered(st):
        ext = hx[st].reshape(4 * BAND, BAND)
        return (wm[...] * dot(bm[...], ext, HIGH)).astype(BF16)

    def small_start(i, block):
        scs[i, 0] = block
        for k in range(1, NY):
            send(scs.at[i, 0], scr.at[i, k], sem_cs.at[i, k], sem_cr.at[i, k], y=yp[k])

    def small_middle(i):
        total = scs[i, 0]
        for k in range(1, NY):
            arrived(scr.at[i, k], sem_cs.at[i, k], sem_cr.at[i, k], y=yp[k])
            total = total + scr[i, k]
        scs[i, 1] = total
        for k in range(1, NZ):
            send(scs.at[i, 1], scr.at[i, NY + k], sem_cs.at[i, NY + k], sem_cr.at[i, NY + k], z=zp[k])

    def small_end(i):
        total = scs[i, 1]
        for k in range(1, NZ):
            arrived(scr.at[i, NY + k], sem_cs.at[i, NY + k], sem_cr.at[i, NY + k], z=zp[k])
            total = total + scr[i, NY + k]
        return total

    half = NZ // 2 * RB

    def scatter(st, w, early, late):
        part = dot(atb[yp[2]], w).reshape(2, NZ // 2, RB, 128)
        for way, peer in ((0, yp[1]), (1, ym[1])):
            sb[st, way, 0] = part[way]
            send(sb.at[st, way, 0], rb.at[st, way, 0], sem_sb.at[st, way, 0], sem_rb.at[st, way, 0], y=peer)
        for way, target, peer in ((0, zp[4], zp[1]), (1, zm[3], zm[1])):
            sa[st, way, 0] = dot(ata[target], w).reshape(NY, RA, 128)
            for j in range(NY):
                send(
                    sa.at[st, way, 0, j], ra.at[st, way, 0, j],
                    sem_sa.at[st, way, 0, j], sem_ra.at[st, way, 0, j], z=peer,
                )
        for way, peer in ((0, yp[1]), (1, ym[1])):
            part = dot(atb[peer], w).reshape(2, NZ // 2, RB, 128)
            sb[st, way, 1] = part[1 - way]
            send(sb.at[st, way, 1], rb.at[st, way, 1], sem_sb.at[st, way, 1], sem_rb.at[st, way, 1], y=peer)
            sb[st, way, 2] = part[way]

        def product(i, carry):
            target = lax.rem(z + 5 + jnp.where(i < 3, 0, 0) + i, NZ)
            y_a[target] = dot(ata[target], w).reshape(NY, RA, 128)
            return carry

        lax.fori_loop(1, NZ - 1, product, 0)
        y_b[...] = dot(atb[y], w).reshape(NZ, RB, 128)
        early()
        for s in range(1, 4):
            for j in range(NY):
                for way, target, peer in ((0, zp[4 - s], zp[1]), (1, zm[3 - s], zm[1])):
                    if way == 1 and s == 3:
                        continue
                    arrived(
                        ra.at[st, way, s - 1, j], sem_sa.at[st, way, s - 1, j], sem_ra.at[st, way, s - 1, j], z=peer
                    )
                    sa[st, way, s, j] = ra[st, way, s - 1, j] + y_a[target, j]
                    send(
                        sa.at[st, way, s, j], ra.at[st, way, s, j],
                        sem_sa.at[st, way, s, j], sem_ra.at[st, way, s, j], z=peer,
                    )
            if s == 1:
                for way, peer in ((0, yp[1]), (1, ym[1])):
                    arrived(rb.at[st, way, 0], sem_sb.at[st, way, 0], sem_rb.at[st, way, 0], y=peer)
                    sb[st, way, 2] = sb[st, way, 2] + rb[st, way, 0]
                    send(
                        sb.at[st, way, 2], rb.at[st, way, 2], sem_sb.at[st, way, 2], sem_rb.at[st, way, 2], y=peer
                    )
                late()
            if s == 2:
                for way, peer in ((0, yp[1]), (1, ym[1])):
                    for kind in (1, 2):
                        arrived(
                            rb.at[st, way, kind], sem_sb.at[st, way, kind], sem_rb.at[st, way, kind], y=peer
                        )
                szb[st, 0 : NZ // 2] = y_b[0 : NZ // 2] + rb[st, 0, 2] + rb[st, 1, 1]
                szb[st, NZ // 2 :] = y_b[NZ // 2 :] + rb[st, 0, 1] + rb[st, 1, 2]
                for k in (4, 3, 5, 2, 6, 1, 7):
                    send(szb.at[st, zp[k]], rzb.at[st, k], sem_szb.at[st, k], sem_rzb.at[st, k], z=zp[k])
        for j in range(NY):
            arrived(ra.at[st, 0, 3, j], sem_sa.at[st, 0, 3, j], sem_ra.at[st, 0, 3, j], z=zp[1])
            arrived(ra.at[st, 1, 2, j], sem_sa.at[st, 1, 2, j], sem_ra.at[st, 1, 2, j], z=zm[1])
            sya[st, j] = ra[st, 0, 3, j] + ra[st, 1, 2, j] + y_a[z, j]
        for k in (2, 1, 3):
            send(sya.at[st, yp[k]], rya.at[st, k], sem_sya.at[st, k], sem_rya.at[st, k], y=yp[k])
        sum_b = szb[st, z]
        for k in range(1, NZ):
            arrived(rzb.at[st, k], sem_szb.at[st, k], sem_rzb.at[st, k], z=zp[k])
            sum_b = sum_b + rzb[st, k]
        sum_a = sya[st, y]
        for k in range(1, NY):
            arrived(rya.at[st, k], sem_sya.at[st, k], sem_rya.at[st, k], y=yp[k])
            sum_a = sum_a + rya[st, k]
        return sum_a, sum_b

    first_half, second_half = (0, 1, 7, 2), (6, 3, 5, 4)

    def gathered_product(it, rows_a, rows_b, middle):
        ga[it, z, y] = rows_a.astype(BF16)
        gb[it, y, z] = rows_b.astype(BF16)

        def put_a(way, s, k):
            zz, yy = (zm[s] if way == 0 else zp[s]), ym[k]
            peer = zp[1] if way == 0 else zm[1]
            send(ga.at[it, zz, yy], ga.at[it, zz, yy], sem_gs.at[it, 0, way, s, k], sem_ga.at[it, way, s, k], z=peer)

        def got_a(way, s, k):
            zz, yy = (zm[s + 1] if way == 0 else zp[s + 1]), ym[k]
            arrived(ga.at[it, zz, yy], sem_gs.at[it, 0, way, s, k], sem_ga.at[it, way, s, k], z=zp[1])

        def put_b(way, s, k):
            zz, yy = zm[k], (ym[s] if way == 0 else yp[s])
            peer = yp[1] if way == 0 else ym[1]
            send(gb.at[it, yy, zz], gb.at[it, yy, zz], sem_gs.at[it, 1, way, s, k], sem_gby.at[it, way, s, k], y=peer)

        def got_b(way, s, k):
            zz, yy = zm[k], (ym[s + 1] if way == 0 else yp[s + 1])
            arrived(gb.at[it, yy, zz], sem_gs.at[it, 1, way, s, k], sem_gby.at[it, way, s, k], y=yp[1])

        for k in (2, 1, 3):
            send(ga.at[it, z, y], ga.at[it, z, y], sem_gs.at[it, 0, 0, 4, k], sem_gay.at[it, k], y=yp[k])
        put_a(0, 0, 0)
        put_a(1, 0, 0)
        for k in (4, 3, 5, 2, 6, 1, 7):
            send(gb.at[it, y, z], gb.at[it, y, z], sem_gs.at[it, 1, 0, 2, k], sem_gb.at[it, k], z=zp[k])
        put_b(0, 0, 0)
        put_b(1, 0, 0)
        for k in (1, 3, 2):
            arrived(ga.at[it, z, ym[k]], sem_gs.at[it, 0, 0, 4, k], sem_gay.at[it, k], y=yp[k])
            put_a(0, 0, k)
            put_a(1, 0, k)
        v = dot(aa[z], ga[it, z].reshape(NY * RA, 128))
        for s in range(1, 4):
            for k in (0, 1, 3, 2):
                got_a(0, s - 1, k)
                put_a(0, s, k)
                got_a(1, s - 1, k)
                if s < 3:
                    put_a(1, s, k)
            if s == 1:
                for k in (1, 7, 2, 6, 3, 5, 4):
                    arrived(gb.at[it, y, zm[k]], sem_gs.at[it, 1, 0, 2, k], sem_gb.at[it, k], z=zp[k])
                    put_b(0, 0, k)
                    put_b(1, 0, k)
            if s == 2:
                for k in first_half:
                    got_b(0, 0, k)
                    put_b(0, 1, k)
                for k in second_half:
                    got_b(1, 0, k)
                    put_b(1, 1, k)
                middle()
            v = v + dot(aa[zm[s]], ga[it, zm[s]].reshape(NY * RA, 128))
            v = v + dot(aa[zp[s]], ga[it, zp[s]].reshape(NY * RA, 128))
        v = v + dot(ab[y], gb[it, y].reshape(NZ * RB, 128))
        for k in second_half:
            got_b(0, 0, k)
        for k in first_half:
            got_b(1, 0, k)
        v = v + dot(ab[yp[1]], gb[it, yp[1]].reshape(NZ * RB, 128))
        v = v + dot(ab[ym[1]], gb[it, ym[1]].reshape(NZ * RB, 128))
        for k in first_half:
            got_b(0, 1, k)
        for k in second_half:
            got_b(1, 1, k)
        v = v + dot(ab[yp[2]], gb[it, yp[2]].reshape(NZ * RB, 128))
        for k in range(NY):
            got_a(0, 3, k)
        return v + dot(aa[zm[4]], ga[it, zm[4]].reshape(NY * RA, 128))

    def slab_values(it, v, scal, finish):
        vs[it] = v.reshape(2, BAND, 128)
        scc[it, 0] = scal
        send(vs.at[it, other], vr.at[it], sem_vs.at[it, 0], sem_vr.at[it, 0], c=other)
        send(scc.at[it, 0], scc.at[it, 1], sem_vs.at[it, 1], sem_vr.at[it, 1], c=other)
        arrived(vr.at[it], sem_vs.at[it, 0], sem_vr.at[it, 0], c=other)
        arrived(scc.at[it, 1], sem_vs.at[it, 1], sem_vr.at[it, 1], c=other)
        us[it, 0:BAND] = vs[it, c] + vr[it]
        us[it, BAND:] = scc[it, 0] + scc[it, 1]
        for k in (2, 1, 3):
            send(us.at[it], ur.at[it, k], sem_us.at[it, k], sem_ur.at[it, k], x=xp[k])
        total = us[it]
        for k in range(1, NX):
            arrived(ur.at[it, k], sem_us.at[it, k], sem_ur.at[it, k], x=xp[k])
            total = total + ur[it, k]
        mask = wm[pl.ds(pl.multiple_of(c * BAND, BAND), BAND), :]
        block, scal = finish(mask * total[0:BAND], total[BAND:])
        hx[it + 1, 1 + c] = block
        slot = 3 - 3 * c
        step = jnp.where(c == 0, t_down, t_up)
        mine = hx.at[it + 1, 1 + c]
        send(mine, mine, sem_hs.at[it + 1, 1 + c], sem_hr.at[it + 1, 1 + c], c=other)
        for core in range(NC):
            send(
                mine, hx.at[it + 1, slot], sem_hs.at[it + 1, 4 + core], sem_hr.at[it + 1, slot],
                z=lax.div(step, NY), y=lax.rem(step, NY), c=jnp.int32(core),
            )
        for place in (2 - c, 0, 3):
            arrived(hx.at[it + 1, place], sem_hs.at[it + 1, 0], sem_hr.at[it + 1, place], c=other)
        return block, scal

    masked = wm[...] * obs[...]
    hx[0, 1] = masked[0:BAND]
    hx[0, 2] = masked[BAND:]
    pl.semaphore_wait(barrier, len(peers))
    send(
        hx.at[0, 2], hx.at[0, 0], sem_hs.at[0, 0], sem_hr.at[0, 0],
        z=lax.div(t_up, NY), y=lax.rem(t_up, NY),
    )
    send(
        hx.at[0, 1], hx.at[0, 3], sem_hs.at[0, 3], sem_hr.at[0, 3],
        z=lax.div(t_down, NY), y=lax.rem(t_down, NY),
    )
    arrived(hx.at[0, 0], sem_hs.at[0, 0], sem_hr.at[0, 0], c=other)
    arrived(hx.at[0, 3], sem_hs.at[0, 3], sem_hr.at[0, 3], c=other)
    nothing = lambda: None
    res_a, res_b = scatter(0, filtered(0), nothing, nothing)

    def col_sum(a, b):
        return jnp.sum(a, 0, keepdims=True) + jnp.sum(b, 0, keepdims=True)

    def rows_of(*rows):
        spare = jnp.zeros((8 - len(rows), 128), F32)
        return jnp.concatenate([*rows, spare], 0)

    dir_a, dir_b = pca[...] * res_a, pcb[...] * res_b
    small_start(0, rows_of(col_sum(res_a * dir_a, res_b * dir_b), col_sum(kda[...] * dir_a * dir_a, kdb[...] * dir_b * dir_b)))
    v = gathered_product(0, dir_a, dir_b, lambda: small_middle(0))
    block, scal = slab_values(0, v, small_end(0), lambda block, scal: (block, scal))
    norm, diag = scal[0:1], scal[1:2]

    def slab_inner(it, w):
        own = hx[it + 1, 1] * w[0:BAND].astype(F32) + hx[it + 1, 2] * w[BAND:].astype(F32)
        return rows_of(jnp.sum(own, 0, keepdims=True))

    w = filtered(1)
    image_a, image_b = scatter(1, w, lambda: small_start(1, slab_inner(0, w)), lambda: small_middle(1))
    step_len = norm / (diag + small_end(1)[0:1])
    image_a, image_b = image_a + kda[...] * dir_a, image_b + kdb[...] * dir_b
    sol_a, sol_b = step_len * dir_a, step_len * dir_b
    res_a, res_b = res_a - step_len * image_a, res_b - step_len * image_b
    scaled_a, scaled_b = pca[...] * res_a, pcb[...] * res_b
    small_start(
        2,
        rows_of(
            col_sum(res_a * scaled_a, res_b * scaled_b),
            col_sum(kda[...] * scaled_a * scaled_a, kdb[...] * scaled_b * scaled_b),
            col_sum(kda[...] * scaled_a * dir_a, kdb[...] * scaled_b * dir_b),
        ),
    )
    v = gathered_product(1, scaled_a, scaled_b, lambda: small_middle(2))

    def finish(new_block, scal):
        ratio = scal[0:1] / norm
        return new_block + ratio * block, scal

    _, scal = slab_values(1, v, small_end(2), finish)
    ratio = scal[0:1] / norm
    norm = scal[0:1]
    diag = scal[1:2] + 2.0 * ratio * scal[2:3] + ratio * ratio * diag
    dir_a, dir_b = scaled_a + ratio * dir_a, scaled_b + ratio * dir_b
    w = filtered(2)
    image_a, image_b = scatter(2, w, lambda: small_start(3, slab_inner(1, w)), lambda: small_middle(3))
    step_len = norm / (diag + small_end(3)[0:1])
    image_a, image_b = image_a + kda[...] * dir_a, image_b + kdb[...] * dir_b
    sol_a, sol_b = sol_a + step_len * dir_a, sol_b + step_len * dir_b
    res_a, res_b = res_a - step_len * image_a, res_b - step_len * image_b
    xout[0:NA] = sol_a[0:NA]
    xout[NA:] = sol_b[0:NB]
    rout[0:NA] = res_a[0:NA]
    rout[NA:] = res_b[0:NB]
    for copy in pending:
        copy.wait_send()


def toeplitz(pattern, band_len):
    tiled = jnp.tile(pattern, band_len)[: band_len * (2 * band_len - 1)]
    return tiled.reshape(band_len, 2 * band_len - 1)[:, :band_len]


def block_pair(filter_taps):
    band_len = filter_taps.shape[0]
    spacer = jnp.zeros((band_len,), jnp.float32)
    reversed_taps = filter_taps[:0:-1]
    lower = jnp.concatenate([filter_taps[:1], spacer, reversed_taps])
    upper = jnp.concatenate([jnp.zeros((1,), jnp.float32), reversed_taps, spacer])
    return (toeplitz(lower, band_len), toeplitz(upper, band_len))


def shards(design, observed, slab_counts, gap_mask, filter_taps, kaula_diag, precond):
    rows = observed.shape[0]
    own = NA + NB
    t = lax.axis_index(TM)
    pieces = design.reshape(rows, NZ, NY, own)
    piece_a = jnp.pad(pieces[..., :NA], ((0, 0), (0, 0), (0, 0), (0, RA - NA)))
    piece_b = jnp.pad(pieces[..., NA:], ((0, 0), (0, 0), (0, 0), (0, RB - NB)))
    aa = piece_a.transpose(1, 0, 2, 3).reshape(NZ, rows, NY * RA)
    ata = piece_a.transpose(1, 2, 3, 0).reshape(NZ, NY * RA, rows)
    ab = piece_b.transpose(2, 0, 1, 3).reshape(NY, rows, NZ * RB)
    atb = piece_b.transpose(2, 1, 3, 0).reshape(NY, NZ * RB, rows)
    position = jnp.arange(rows, dtype=jnp.int32)
    weight = ((gap_mask == 1) & (position < slab_counts[0])).astype(F32)
    wm = jnp.broadcast_to(weight[:, None], (rows, 128))
    lo, up = block_pair(filter_taps)

    def owned(diag):
        mine = lax.dynamic_slice_in_dim(diag, t * own, own, 0)
        part_a = jnp.pad(mine[:NA], (0, RA - NA))
        part_b = jnp.pad(mine[NA:], (0, RB - NB))
        return (
            jnp.broadcast_to(part_a[:, None], (RA, 128)),
            jnp.broadcast_to(part_b[:, None], (RB, 128)),
        )

    kda, kdb = owned(kaula_diag)
    pca, pcb = owned(precond)
    dma = pltpu.SemaphoreType.DMA
    args = (aa, ab, ata, atb, observed, wm, lo, up, lo.T, up.T, kda, kdb, pca, pcb)
    vm = pltpu.VMEM
    scratch = [
        vm((2 * BAND, 4 * BAND), F32),
        vm((NZ, NY, RA, 128), F32),
        vm((NZ, RB, 128), F32),
        vm((3, 2, 4, NY, RA, 128), F32),
        vm((3, 2, 4, NY, RA, 128), F32),
        vm((3, NY, RA, 128), F32),
        vm((3, NY, RA, 128), F32),
        vm((3, 2, 3, NZ // 2, RB, 128), F32),
        vm((3, 2, 3, NZ // 2, RB, 128), F32),
        vm((3, NZ, RB, 128), F32),
        vm((3, NZ, RB, 128), F32),
        vm((2, NZ, NY, RA, 128), BF16),
        vm((2, NY, NZ, RB, 128), BF16),
        vm((2, 2, BAND, 128), F32),
        vm((2, BAND, 128), F32),
        vm((2, BAND + 8, 128), F32),
        vm((2, NX, BAND + 8, 128), F32),
        vm((3, 4, BAND, 128), F32),
        vm((4, 2, 8, 128), F32),
        vm((4, NY + NZ, 8, 128), F32),
        vm((2, 2, 8, 128), F32),
        dma((3, 2, 4, NY)), dma((3, 2, 4, NY)), dma((3, NY)), dma((3, NY)),
        dma((3, 2, 3)), dma((3, 2, 3)), dma((3, NZ)), dma((3, NZ)),
        dma((2, 2, 2, 5, NZ)), dma((2, 2, 4, NY)), dma((2, NY)), dma((2, NZ)), dma((2, 2, 2, NZ)),
        dma((2, 2)), dma((2, 2)), dma((2, NX)), dma((2, NX)), dma((3, 6)), dma((3, 4)),
        dma((4, NY + NZ)), dma((4, NY + NZ)),
    ]
    out = jax.ShapeDtypeStruct((own, 128), F32)
    return pl.pallas_call(
        kernel,
        name="cg",
        out_shape=(out, out),
        in_specs=[pl.BlockSpec(memory_space=vm)] * len(args),
        out_specs=(pl.BlockSpec(memory_space=vm),) * 2,
        scratch_shapes=scratch,
        compiler_params=pltpu.CompilerParams(
            collective_id=0, has_side_effects=True, vmem_limit_bytes=60 * 1024 * 1024
        ),
    )(*args)


def solution(mesh):
    torus = Mesh(mesh.devices.reshape(NZ, NY, NX, NC), AXES)
    in_specs = (P(TM, COEF), P(TM, None), P(TM), P(TM), P(), P(COEF), P(COEF))
    out_specs = (P((*COEF, *TM), None),) * 2
    return jax.shard_map(shards, mesh=torus, in_specs=in_specs, out_specs=out_specs, check_vma=False)
```

```python
import functools

import jax
import jax.numpy as jnp
from jax import lax
from jax.experimental import pallas as pl
from jax.experimental.pallas import tpu as pltpu
from jax.sharding import Mesh
from jax.sharding import PartitionSpec as P

AXES = ("z", "y", "x", "c")
TM = ("z", "y")
COEF = ("x", "c")
MESH = pl.DeviceIdType.MESH
NZ, NY, NX, NC = 8, 4, 4, 2
NA, NB = 92, 104
RA, RB = 96, 112
OWN = NA + NB
LANES = 128
WIDE = 3 * LANES
I16 = jnp.int16
I32 = jnp.int32
BAND = 128
F32 = jnp.float32
BF16 = jnp.bfloat16
HIGH = lax.Precision.HIGHEST


def dot(a, b, precision=None):
    return jnp.dot(a, b, preferred_element_type=F32, precision=precision)


def dot_t(a, b, precision=None):
    return lax.dot_general(a, b, (((1,), (1,)), ((), ())), preferred_element_type=F32, precision=precision)


def encoded(v, spare):
    top = jnp.maximum(jnp.max(jnp.abs(v), axis=-2, keepdims=True), 1e-30)
    power = jnp.floor(jnp.log2(top)) + 1.0
    q = jnp.clip(jnp.round(v * jnp.exp2(15.0 - power)), -32767.0, 32767.0)
    row = lax.broadcasted_iota(I32, v.shape, v.ndim - 2)
    return jnp.where(row == spare, power, q).astype(I32).astype(I16)


def decoded(q, spare):
    v = q.astype(I32).astype(F32)
    return v * jnp.exp2(v[..., spare : spare + 1, :] - 15.0)


def enc_a(v):
    return encoded(v, NA)


def enc_b(v):
    return encoded(v, NB)


def dec_a(q):
    return decoded(q, NA)


def dec_b(q):
    return decoded(q, NB)


def rcopy(src, dst, ssem, rsem, **device):
    return pltpu.make_async_remote_copy(
        src_ref=src, dst_ref=dst, send_sem=ssem, recv_sem=rsem, device_id=device, device_id_type=MESH
    )


def kernel(
    design, obs, counts, gaps, taps, kaula, precond,
    xout, rout,
    aa, ab, ata, atb, wm, kda, kdb, pca, pcb, column, bm, y_a, y_b, y_c,
    sa, ra, sya, rya, sb, rb, szb, rzb,
    ga, gb, vs, vr, us, ur, hx, scs, scr, scc,
    sem_sa, sem_ra, sem_sya, sem_rya, sem_sb, sem_rb, sem_szb, sem_rzb,
    sem_gs, sem_ga, sem_gay, sem_gb, sem_gby,
    sem_vs, sem_vr, sem_us, sem_ur, sem_hs, sem_hr, sem_cs, sem_cr,
):
    z, y, x, c = (lax.axis_index(name) for name in AXES)
    t = z * NY + y
    zp = [lax.rem(z + k, NZ) for k in range(NZ)]
    zm = [lax.rem(z + NZ - k, NZ) for k in range(NZ)]
    yp = [lax.rem(y + k, NY) for k in range(NY)]
    ym = [lax.rem(y + NY - k, NY) for k in range(NY)]
    xp = [lax.rem(x + k, NX) for k in range(NX)]
    other = 1 - c
    t_up = lax.rem(t + 1, NZ * NY)
    t_down = lax.rem(t + NZ * NY - 1, NZ * NY)
    pending = []

    def send(src, dst, ssem, rsem, **device):
        copy = rcopy(src, dst, ssem, rsem, **device)
        copy.start()
        pending.append(copy)

    def arrived(dst, ssem, rsem, **device):
        rcopy(dst, dst, ssem, rsem, **device).wait_recv()

    barrier = pltpu.get_barrier_semaphore()
    peers = [dict(z=zp[k]) for k in range(1, NZ)] + [dict(y=yp[k]) for k in range(1, NY)]
    peers += [dict(x=xp[k]) for k in range(1, NX)] + [dict(c=other)]
    for step in (t_up, t_down):
        for core in range(NC):
            peers.append(dict(z=lax.div(step, NY), y=lax.rem(step, NY), c=jnp.int32(core)))
    for peer in peers:
        pl.semaphore_signal(barrier, inc=1, device_id=peer, device_id_type=MESH)

    keep_first = jnp.where(t == 0, 0.0, 1.0).astype(F32)
    keep_last = jnp.where(t == NZ * NY - 1, 0.0, 1.0).astype(F32)
    row = lax.broadcasted_iota(I32, (BAND, BAND), 0)
    col = lax.broadcasted_iota(I32, (BAND, BAND), 1)
    rolled = pltpu.roll(jnp.broadcast_to(taps[...], (BAND, BAND)), 0, 1, stride=1, stride_axis=0)
    lot = jnp.where(col >= row, rolled, 0.0)
    upt = jnp.where(col < row, rolled, 0.0)
    ll = dot_t(lot, lot, HIGH)
    uu = dot_t(upt, upt, HIGH)
    lu = dot_t(lot, upt, HIGH)
    ul = dot_t(upt, lot, HIGH)
    zero = jnp.zeros((BAND, BAND), F32)
    bm[0:BAND, 0:BAND] = keep_first * lu
    bm[0:BAND, BAND : 2 * BAND] = ll + uu
    bm[0:BAND, 2 * BAND : 3 * BAND] = ul
    bm[0:BAND, 3 * BAND :] = zero
    bm[BAND:, 0:BAND] = zero
    bm[BAND:, BAND : 2 * BAND] = lu
    bm[BAND:, 2 * BAND : 3 * BAND] = ll + keep_last * uu
    bm[BAND:, 3 * BAND :] = keep_last * ul

    for b in range(2):
        on = (gaps[b : b + 1, :] == 1) & (col[0:1] + b * BAND < counts[0])
        wm[b * BAND : (b + 1) * BAND] = jnp.broadcast_to(jnp.where(on, 1.0, 0.0), (BAND, BAND)).T

    line = lax.div(t * OWN, LANES)
    shift = t * OWN - line * LANES
    for diag, part_a, part_b in ((kaula, kda, kdb), (precond, pca, pcb)):
        for k in range(3):
            values = diag[pl.ds(jnp.minimum(line + k, diag.shape[0] - 1), 1), :]
            column[k * LANES : (k + 1) * LANES] = jnp.broadcast_to(values, (LANES, LANES)).T
        row_a = lax.broadcasted_iota(I32, (RA, LANES), 0)
        row_b = lax.broadcasted_iota(I32, (RB, LANES), 0)
        part_a[...] = jnp.where(row_a < NA, column[pl.ds(shift, RA), :], 0.0)
        part_b[...] = jnp.where(row_b < NB, column[pl.ds(shift + NA, RB), :], 0.0)

    def picked(p):
        first = jnp.minimum(lax.div(p * OWN, LANES), design.shape[1] // LANES - 3)
        window = design[:, pl.ds(pl.multiple_of(first * LANES, LANES), WIDE)]
        place = lax.broadcasted_iota(I32, (2 * LANES, WIDE), 0)
        wanted = jnp.where(place < LANES, place, place - LANES + NA)
        real = ((place < NA) | (place >= LANES)) & (place < LANES + NB)
        at = lax.broadcasted_iota(I32, (2 * LANES, WIDE), 1) - (p * OWN - first * LANES)
        return window, jnp.where((at == wanted) & real, 1.0, 0.0).astype(BF16)

    def put_rows(p, carry):
        window, pick = picked(p)
        rows = dot_t(pick, window).astype(BF16)
        zz, yy = lax.div(p, NY), lax.rem(p, NY)
        ata[zz, yy] = rows[0:RA]
        atb[yy, zz] = rows[LANES : LANES + RB]
        return carry

    def put_columns(p, carry):
        window, pick = picked(p)
        columns = dot_t(window, pick).astype(BF16)
        zz, yy = lax.div(p, NY), lax.rem(p, NY)
        aa[zz, :, pl.ds(pl.multiple_of(yy * LANES, LANES), LANES)] = columns[:, 0:LANES]
        ab[yy, :, pl.ds(pl.multiple_of(zz * LANES, LANES), LANES)] = columns[:, LANES:]
        for it in range(2):
            ga[it, zz, yy, RA:] = jnp.zeros((LANES - RA, LANES), BF16)
            gb[it, yy, zz, RB:] = jnp.zeros((LANES - RB, LANES), BF16)
        return carry

    lax.fori_loop(0, NZ * NY, put_rows, 0)

    def at_a(target):
        return ata[target].reshape(NY * RA, 2 * BAND)

    def at_b(target):
        return atb[target].reshape(NZ * RB, 2 * BAND)

    def filtered(st):
        ext = hx[st].reshape(4 * BAND, BAND)
        return (wm[...] * dot(bm[...], ext, HIGH)).astype(BF16)

    def small_start(i, block):
        scs[i, 0] = block
        for k in range(1, NY):
            send(scs.at[i, 0], scr.at[i, k], sem_cs.at[i, k], sem_cr.at[i, k], y=yp[k])

    def small_middle(i):
        total = scs[i, 0]
        for k in range(1, NY):
            arrived(scr.at[i, k], sem_cs.at[i, k], sem_cr.at[i, k], y=yp[k])
            total = total + scr[i, k]
        scs[i, 1] = total
        for k in range(1, NZ):
            send(scs.at[i, 1], scr.at[i, NY + k], sem_cs.at[i, NY + k], sem_cr.at[i, NY + k], z=zp[k])

    def small_end(i):
        total = scs[i, 1]
        for k in range(1, NZ):
            arrived(scr.at[i, NY + k], sem_cs.at[i, NY + k], sem_cr.at[i, NY + k], z=zp[k])
            total = total + scr[i, NY + k]
        return total

    half = NZ // 2 * RB

    def scatter(st, w, early, late):
        part = dot(at_b(yp[2]), w).reshape(2, NZ // 2, RB, 128)
        for way, peer in ((0, yp[1]), (1, ym[1])):
            sb[st, way, 0] = enc_b(part[way])
            send(sb.at[st, way, 0], rb.at[st, way, 0], sem_sb.at[st, way, 0], sem_rb.at[st, way, 0], y=peer)
        for way, target, peer in ((0, zp[4], zp[1]), (1, zm[3], zm[1])):
            sa[st, way, 0] = enc_a(dot(at_a(target), w).reshape(NY, RA, 128))
            for j in range(NY):
                send(
                    sa.at[st, way, 0, j], ra.at[st, way, 0, j],
                    sem_sa.at[st, way, 0, j], sem_ra.at[st, way, 0, j], z=peer,
                )
        for way, peer in ((0, yp[1]), (1, ym[1])):
            part = dot(at_b(peer), w).reshape(2, NZ // 2, RB, 128)
            sb[st, way, 1] = enc_b(part[1 - way])
            send(sb.at[st, way, 1], rb.at[st, way, 1], sem_sb.at[st, way, 1], sem_rb.at[st, way, 1], y=peer)
            y_c[way] = part[way]

        def product(i, carry):
            target = lax.rem(z + 5 + i, NZ)
            y_a[target] = dot(at_a(target), w).reshape(NY, RA, 128)
            return carry

        lax.fori_loop(1, NZ - 1, product, 0)
        y_b[...] = dot(at_b(y), w).reshape(NZ, RB, 128)
        early()
        for s in range(1, 4):
            for j in range(NY):
                for way, target, peer in ((0, zp[4 - s], zp[1]), (1, zm[3 - s], zm[1])):
                    if way == 1 and s == 3:
                        continue
                    arrived(
                        ra.at[st, way, s - 1, j], sem_sa.at[st, way, s - 1, j], sem_ra.at[st, way, s - 1, j], z=peer
                    )
                    sa[st, way, s, j] = enc_a(dec_a(ra[st, way, s - 1, j]) + y_a[target, j])
                    send(
                        sa.at[st, way, s, j], ra.at[st, way, s, j],
                        sem_sa.at[st, way, s, j], sem_ra.at[st, way, s, j], z=peer,
                    )
            if s == 1:
                for way, peer in ((0, yp[1]), (1, ym[1])):
                    arrived(rb.at[st, way, 0], sem_sb.at[st, way, 0], sem_rb.at[st, way, 0], y=peer)
                    sb[st, way, 2] = enc_b(y_c[way] + dec_b(rb[st, way, 0]))
                    send(
                        sb.at[st, way, 2], rb.at[st, way, 2], sem_sb.at[st, way, 2], sem_rb.at[st, way, 2], y=peer
                    )
                late()
            if s == 2:
                for way, peer in ((0, yp[1]), (1, ym[1])):
                    for kind in (1, 2):
                        arrived(
                            rb.at[st, way, kind], sem_sb.at[st, way, kind], sem_rb.at[st, way, kind], y=peer
                        )
                low = y_b[0 : NZ // 2] + dec_b(rb[st, 0, 2]) + dec_b(rb[st, 1, 1])
                y_b[0 : NZ // 2] = low
                szb[st, 0 : NZ // 2] = enc_b(low)
                high = y_b[NZ // 2 :] + dec_b(rb[st, 0, 1]) + dec_b(rb[st, 1, 2])
                y_b[NZ // 2 :] = high
                szb[st, NZ // 2 :] = enc_b(high)
                for k in (4, 3, 5, 2, 6, 1, 7):
                    send(szb.at[st, zp[k]], rzb.at[st, k], sem_szb.at[st, k], sem_rzb.at[st, k], z=zp[k])
        for j in range(NY):
            arrived(ra.at[st, 0, 3, j], sem_sa.at[st, 0, 3, j], sem_ra.at[st, 0, 3, j], z=zp[1])
            arrived(ra.at[st, 1, 2, j], sem_sa.at[st, 1, 2, j], sem_ra.at[st, 1, 2, j], z=zm[1])
            total = dec_a(ra[st, 0, 3, j]) + dec_a(ra[st, 1, 2, j]) + y_a[z, j]
            y_a[z, j] = total
            sya[st, j] = enc_a(total)
        for k in (2, 1, 3):
            send(sya.at[st, yp[k]], rya.at[st, k], sem_sya.at[st, k], sem_rya.at[st, k], y=yp[k])
        sum_b = y_b[z]
        for k in range(1, NZ):
            arrived(rzb.at[st, k], sem_szb.at[st, k], sem_rzb.at[st, k], z=zp[k])
            sum_b = sum_b + dec_b(rzb[st, k])
        sum_a = y_a[z, y]
        for k in range(1, NY):
            arrived(rya.at[st, k], sem_sya.at[st, k], sem_rya.at[st, k], y=yp[k])
            sum_a = sum_a + dec_a(rya[st, k])
        return sum_a, sum_b

    first_half, second_half = (0, 1, 7, 2), (6, 3, 5, 4)

    def gathered_product(it, rows_a, rows_b, middle):
        ga[it, z, y, 0:RA] = rows_a.astype(BF16)
        gb[it, y, z, 0:RB] = rows_b.astype(BF16)

        def part_a(it, zz, yy):
            return ga.at[it, zz, yy, pl.ds(0, RA)]

        def part_b(it, yy, zz):
            return gb.at[it, yy, zz, pl.ds(0, RB)]

        def put_a(way, s, k):
            zz, yy = (zm[s] if way == 0 else zp[s]), ym[k]
            peer = zp[1] if way == 0 else zm[1]
            send(part_a(it, zz, yy), part_a(it, zz, yy), sem_gs.at[it, 0, way, s, k], sem_ga.at[it, way, s, k], z=peer)

        def got_a(way, s, k):
            zz, yy = (zm[s + 1] if way == 0 else zp[s + 1]), ym[k]
            arrived(part_a(it, zz, yy), sem_gs.at[it, 0, way, s, k], sem_ga.at[it, way, s, k], z=zp[1])

        def put_b(way, s, k):
            zz, yy = zm[k], (ym[s] if way == 0 else yp[s])
            peer = yp[1] if way == 0 else ym[1]
            send(part_b(it, yy, zz), part_b(it, yy, zz), sem_gs.at[it, 1, way, s, k], sem_gby.at[it, way, s, k], y=peer)

        def got_b(way, s, k):
            zz, yy = zm[k], (ym[s + 1] if way == 0 else yp[s + 1])
            arrived(part_b(it, yy, zz), sem_gs.at[it, 1, way, s, k], sem_gby.at[it, way, s, k], y=yp[1])

        for k in (2, 1, 3):
            send(part_a(it, z, y), part_a(it, z, y), sem_gs.at[it, 0, 0, 4, k], sem_gay.at[it, k], y=yp[k])
        put_a(0, 0, 0)
        put_a(1, 0, 0)
        for k in (4, 3, 5, 2, 6, 1, 7):
            send(part_b(it, y, z), part_b(it, y, z), sem_gs.at[it, 1, 0, 2, k], sem_gb.at[it, k], z=zp[k])
        put_b(0, 0, 0)
        put_b(1, 0, 0)
        for k in (1, 3, 2):
            arrived(part_a(it, z, ym[k]), sem_gs.at[it, 0, 0, 4, k], sem_gay.at[it, k], y=yp[k])
            put_a(0, 0, k)
            put_a(1, 0, k)
        v = dot(aa[z], ga[it, z].reshape(NY * LANES, LANES))
        for s in range(1, 4):
            for k in (0, 1, 3, 2):
                got_a(0, s - 1, k)
                put_a(0, s, k)
                got_a(1, s - 1, k)
                if s < 3:
                    put_a(1, s, k)
            if s == 1:
                for k in (1, 7, 2, 6, 3, 5, 4):
                    arrived(part_b(it, y, zm[k]), sem_gs.at[it, 1, 0, 2, k], sem_gb.at[it, k], z=zp[k])
                    put_b(0, 0, k)
                    put_b(1, 0, k)
            if s == 2:
                for k in first_half:
                    got_b(0, 0, k)
                    put_b(0, 1, k)
                for k in second_half:
                    got_b(1, 0, k)
                    put_b(1, 1, k)
                middle()
            v = v + dot(aa[zm[s]], ga[it, zm[s]].reshape(NY * LANES, LANES))
            v = v + dot(aa[zp[s]], ga[it, zp[s]].reshape(NY * LANES, LANES))
        v = v + dot(ab[y], gb[it, y].reshape(NZ * LANES, LANES))
        for k in second_half:
            got_b(0, 0, k)
        for k in first_half:
            got_b(1, 0, k)
        v = v + dot(ab[yp[1]], gb[it, yp[1]].reshape(NZ * LANES, LANES))
        v = v + dot(ab[ym[1]], gb[it, ym[1]].reshape(NZ * LANES, LANES))
        for k in first_half:
            got_b(0, 1, k)
        for k in second_half:
            got_b(1, 1, k)
        v = v + dot(ab[yp[2]], gb[it, yp[2]].reshape(NZ * LANES, LANES))
        for k in range(NY):
            got_a(0, 3, k)
        return v + dot(aa[zm[4]], ga[it, zm[4]].reshape(NY * LANES, LANES))

    def slab_values(it, v, scal, finish):
        vs[it] = v.reshape(2, BAND, 128)
        scc[it, 0] = scal
        send(vs.at[it, other], vr.at[it], sem_vs.at[it, 0], sem_vr.at[it, 0], c=other)
        send(scc.at[it, 0], scc.at[it, 1], sem_vs.at[it, 1], sem_vr.at[it, 1], c=other)
        arrived(vr.at[it], sem_vs.at[it, 0], sem_vr.at[it, 0], c=other)
        arrived(scc.at[it, 1], sem_vs.at[it, 1], sem_vr.at[it, 1], c=other)
        us[it, 0:BAND] = vs[it, c] + vr[it]
        us[it, BAND:] = scc[it, 0] + scc[it, 1]
        for k in (2, 1, 3):
            send(us.at[it], ur.at[it, k], sem_us.at[it, k], sem_ur.at[it, k], x=xp[k])
        total = us[it]
        for k in range(1, NX):
            arrived(ur.at[it, k], sem_us.at[it, k], sem_ur.at[it, k], x=xp[k])
            total = total + ur[it, k]
        mask = wm[pl.ds(pl.multiple_of(c * BAND, BAND), BAND), :]
        block, scal = finish(mask * total[0:BAND], total[BAND:])
        hx[it + 1, 1 + c] = block
        slot = 3 - 3 * c
        step = jnp.where(c == 0, t_down, t_up)
        mine = hx.at[it + 1, 1 + c]
        send(mine, mine, sem_hs.at[it + 1, 1 + c], sem_hr.at[it + 1, 1 + c], c=other)
        for core in range(NC):
            send(
                mine, hx.at[it + 1, slot], sem_hs.at[it + 1, 4 + core], sem_hr.at[it + 1, slot],
                z=lax.div(step, NY), y=lax.rem(step, NY), c=jnp.int32(core),
            )
        for place in (2 - c, 0, 3):
            arrived(hx.at[it + 1, place], sem_hs.at[it + 1, 0], sem_hr.at[it + 1, place], c=other)
        return block, scal

    masked = wm[...] * obs[...]
    hx[0, 1] = masked[0:BAND]
    hx[0, 2] = masked[BAND:]
    pl.semaphore_wait(barrier, len(peers))
    send(
        hx.at[0, 2], hx.at[0, 0], sem_hs.at[0, 0], sem_hr.at[0, 0],
        z=lax.div(t_up, NY), y=lax.rem(t_up, NY),
    )
    send(
        hx.at[0, 1], hx.at[0, 3], sem_hs.at[0, 3], sem_hr.at[0, 3],
        z=lax.div(t_down, NY), y=lax.rem(t_down, NY),
    )
    arrived(hx.at[0, 0], sem_hs.at[0, 0], sem_hr.at[0, 0], c=other)
    arrived(hx.at[0, 3], sem_hs.at[0, 3], sem_hr.at[0, 3], c=other)
    nothing = lambda: None
    res_a, res_b = scatter(0, filtered(0), lambda: lax.fori_loop(0, NZ * NY, put_columns, 0), nothing)

    def col_sum(a, b):
        return jnp.sum(a, 0, keepdims=True) + jnp.sum(b, 0, keepdims=True)

    def rows_of(*rows):
        spare = jnp.zeros((8 - len(rows), 128), F32)
        return jnp.concatenate([*rows, spare], 0)

    dir_a, dir_b = pca[...] * res_a, pcb[...] * res_b
    small_start(0, rows_of(col_sum(res_a * dir_a, res_b * dir_b), col_sum(kda[...] * dir_a * dir_a, kdb[...] * dir_b * dir_b)))
    v = gathered_product(0, dir_a, dir_b, lambda: small_middle(0))
    block, scal = slab_values(0, v, small_end(0), lambda block, scal: (block, scal))
    norm, diag = scal[0:1], scal[1:2]

    def slab_inner(it, w):
        own = hx[it + 1, 1] * w[0:BAND].astype(F32) + hx[it + 1, 2] * w[BAND:].astype(F32)
        return rows_of(jnp.sum(own, 0, keepdims=True))

    w = filtered(1)
    image_a, image_b = scatter(1, w, lambda: small_start(1, slab_inner(0, w)), lambda: small_middle(1))
    step_len = norm / (diag + small_end(1)[0:1])
    image_a, image_b = image_a + kda[...] * dir_a, image_b + kdb[...] * dir_b
    sol_a, sol_b = step_len * dir_a, step_len * dir_b
    res_a, res_b = res_a - step_len * image_a, res_b - step_len * image_b
    scaled_a, scaled_b = pca[...] * res_a, pcb[...] * res_b
    small_start(
        2,
        rows_of(
            col_sum(res_a * scaled_a, res_b * scaled_b),
            col_sum(kda[...] * scaled_a * scaled_a, kdb[...] * scaled_b * scaled_b),
            col_sum(kda[...] * scaled_a * dir_a, kdb[...] * scaled_b * dir_b),
        ),
    )
    v = gathered_product(1, scaled_a, scaled_b, lambda: small_middle(2))

    def finish(new_block, scal):
        ratio = scal[0:1] / norm
        return new_block + ratio * block, scal

    _, scal = slab_values(1, v, small_end(2), finish)
    ratio = scal[0:1] / norm
    norm = scal[0:1]
    diag = scal[1:2] + 2.0 * ratio * scal[2:3] + ratio * ratio * diag
    dir_a, dir_b = scaled_a + ratio * dir_a, scaled_b + ratio * dir_b
    w = filtered(2)
    image_a, image_b = scatter(2, w, lambda: small_start(3, slab_inner(1, w)), lambda: small_middle(3))
    step_len = norm / (diag + small_end(3)[0:1])
    image_a, image_b = image_a + kda[...] * dir_a, image_b + kdb[...] * dir_b
    sol_a, sol_b = sol_a + step_len * dir_a, sol_b + step_len * dir_b
    res_a, res_b = res_a - step_len * image_a, res_b - step_len * image_b
    xout[0:NA] = sol_a[0:NA]
    xout[NA:] = sol_b[0:NB]
    rout[0:NA] = res_a[0:NA]
    rout[NA:] = res_b[0:NB]
    for copy in pending:
        copy.wait_send()


def shards(design, observed, slab_counts, gap_mask, filter_taps, kaula_diag, precond):
    rows = observed.shape[0]
    coefs = design.shape[1]
    dma = pltpu.SemaphoreType.DMA
    args = (
        design, observed, slab_counts, gap_mask.reshape(rows // LANES, LANES), filter_taps.reshape(1, LANES),
        kaula_diag.reshape(coefs // LANES, LANES), precond.reshape(coefs // LANES, LANES),
    )
    vm = pltpu.VMEM
    scratch = [
        vm((NZ, rows, NY * LANES), BF16),
        vm((NY, rows, NZ * LANES), BF16),
        vm((NZ, NY, RA, rows), BF16),
        vm((NY, NZ, RB, rows), BF16),
        vm((rows, LANES), F32),
        vm((RA, LANES), F32), vm((RB, LANES), F32), vm((RA, LANES), F32), vm((RB, LANES), F32),
        vm((4 * LANES, LANES), F32),
        vm((2 * BAND, 4 * BAND), F32),
        vm((NZ, NY, RA, 128), F32),
        vm((NZ, RB, 128), F32),
        vm((2, NZ // 2, RB, 128), F32),
        vm((3, 2, 4, NY, RA, 128), I16),
        vm((3, 2, 4, NY, RA, 128), I16),
        vm((3, NY, RA, 128), I16),
        vm((3, NY, RA, 128), I16),
        vm((3, 2, 3, NZ // 2, RB, 128), I16),
        vm((3, 2, 3, NZ // 2, RB, 128), I16),
        vm((3, NZ, RB, 128), I16),
        vm((3, NZ, RB, 128), I16),
        vm((2, NZ, NY, LANES, LANES), BF16),
        vm((2, NY, NZ, LANES, LANES), BF16),
        vm((2, 2, BAND, 128), F32),
        vm((2, BAND, 128), F32),
        vm((2, BAND + 8, 128), F32),
        vm((2, NX, BAND + 8, 128), F32),
        vm((3, 4, BAND, 128), F32),
        vm((4, 2, 8, 128), F32),
        vm((4, NY + NZ, 8, 128), F32),
        vm((2, 2, 8, 128), F32),
        dma((3, 2, 4, NY)), dma((3, 2, 4, NY)), dma((3, NY)), dma((3, NY)),
        dma((3, 2, 3)), dma((3, 2, 3)), dma((3, NZ)), dma((3, NZ)),
        dma((2, 2, 2, 5, NZ)), dma((2, 2, 4, NY)), dma((2, NY)), dma((2, NZ)), dma((2, 2, 2, NZ)),
        dma((2, 2)), dma((2, 2)), dma((2, NX)), dma((2, NX)), dma((3, 6)), dma((3, 4)),
        dma((4, NY + NZ)), dma((4, NY + NZ)),
    ]
    out = jax.ShapeDtypeStruct((OWN, LANES), F32)
    return pl.pallas_call(
        kernel,
        name="cg",
        out_shape=(out, out),
        in_specs=[pl.BlockSpec(memory_space=pltpu.SMEM if i == 2 else vm) for i in range(len(args))],
        out_specs=(pl.BlockSpec(memory_space=vm),) * 2,
        scratch_shapes=scratch,
        compiler_params=pltpu.CompilerParams(
            collective_id=0, has_side_effects=True, vmem_limit_bytes=60 * 1024 * 1024
        ),
    )(*args)


def solution(mesh):
    torus = Mesh(mesh.devices.reshape(NZ, NY, NX, NC), AXES)
    in_specs = (P(TM, COEF), P(TM, None), P(TM), P(TM), P(), P(COEF), P(COEF))
    out_specs = (P((*COEF, *TM), None),) * 2
    return jax.shard_map(shards, mesh=torus, in_specs=in_specs, out_specs=out_specs, check_vma=False)
```

```python
import functools

import jax
import jax.numpy as jnp
from jax import lax
from jax.experimental import pallas as pl
from jax.experimental.pallas import tpu as pltpu
from jax.sharding import Mesh
from jax.sharding import PartitionSpec as P

AXES = ("z", "y", "x", "c")
TM = ("z", "y")
COEF = ("x", "c")
MESH = pl.DeviceIdType.MESH
NZ, NY, NX, NC = 8, 4, 4, 2
NA, NB = 92, 104
RA, RB = 96, 112
OWN = NA + NB
LANES = 128
WIDE = 3 * LANES
I16 = jnp.int16
I32 = jnp.int32
BAND = 128
F32 = jnp.float32
BF16 = jnp.bfloat16
HIGH = lax.Precision.HIGHEST


def dot(a, b, precision=None):
    return jnp.dot(a, b, preferred_element_type=F32, precision=precision)


def dot_t(a, b, precision=None):
    return lax.dot_general(a, b, (((1,), (1,)), ((), ())), preferred_element_type=F32, precision=precision)


def encoded(v, spare):
    top = jnp.maximum(jnp.max(jnp.abs(v), axis=-2, keepdims=True), 1e-30)
    power = jnp.floor(jnp.log2(top)) + 1.0
    q = jnp.clip(jnp.round(v * jnp.exp2(15.0 - power)), -32767.0, 32767.0)
    row = lax.broadcasted_iota(I32, v.shape, v.ndim - 2)
    return jnp.where(row == spare, power, q).astype(I32).astype(I16)


def decoded(q, spare):
    v = q.astype(I32).astype(F32)
    return v * jnp.exp2(v[..., spare : spare + 1, :] - 15.0)


def enc_a(v):
    return encoded(v, NA)


def enc_b(v):
    return encoded(v, NB)


def dec_a(q):
    return decoded(q, NA)


def dec_b(q):
    return decoded(q, NB)


def enc_v(v):
    return encoded(jnp.concatenate([v, jnp.zeros((16, LANES), F32)], 0), BAND)


def dec_v(q):
    return decoded(q, BAND)[..., 0:BAND, :]


def rcopy(src, dst, ssem, rsem, **device):
    return pltpu.make_async_remote_copy(
        src_ref=src, dst_ref=dst, send_sem=ssem, recv_sem=rsem, device_id=device, device_id_type=MESH
    )


def kernel(
    design, obs, counts, gaps, taps, kaula, precond,
    xout, rout,
    aa, ab, ata, atb, wm, kda, kdb, pca, pcb, column, bm, y_a, y_b, y_c,
    sa, ra, sya, rya, sb, rb, szb, rzb,
    ga, gb, vs, vr, us, ur, hq, scs, scr, scc, scx,
    sem_sa, sem_ra, sem_sya, sem_rya, sem_sb, sem_rb, sem_szb, sem_rzb,
    sem_gs, sem_ga, sem_gay, sem_gb, sem_gby,
    sem_vs, sem_vr, sem_us, sem_ur, sem_uc, sem_hs, sem_hr, sem_cs, sem_cr,
):
    z, y, x, c = (lax.axis_index(name) for name in AXES)
    t = z * NY + y
    zp = [lax.rem(z + k, NZ) for k in range(NZ)]
    zm = [lax.rem(z + NZ - k, NZ) for k in range(NZ)]
    yp = [lax.rem(y + k, NY) for k in range(NY)]
    ym = [lax.rem(y + NY - k, NY) for k in range(NY)]
    xp = [lax.rem(x + k, NX) for k in range(NX)]
    other = 1 - c
    t_up = lax.rem(t + 1, NZ * NY)
    t_down = lax.rem(t + NZ * NY - 1, NZ * NY)
    pending = []

    def send(src, dst, ssem, rsem, **device):
        rcopy(src, dst, ssem, rsem, **device).start()

    def sent(ref, sem):
        pending.append(rcopy(ref, ref, sem, sem, c=other))

    def arrived(dst, ssem, rsem, **device):
        rcopy(dst, dst, ssem, rsem, **device).wait_recv()

    barrier = pltpu.get_barrier_semaphore()
    peers = [dict(z=zp[k]) for k in range(1, NZ)] + [dict(y=yp[k]) for k in range(1, NY)]
    peers += [dict(x=xp[k]) for k in range(1, NX)] + [dict(c=other)]
    for step in (t_up, t_down):
        for core in range(NC):
            peers.append(dict(z=lax.div(step, NY), y=lax.rem(step, NY), c=jnp.int32(core)))
    for peer in peers:
        pl.semaphore_signal(barrier, inc=1, device_id=peer, device_id_type=MESH)

    row = lax.broadcasted_iota(I32, (BAND, BAND), 0)
    col = lax.broadcasted_iota(I32, (BAND, BAND), 1)
    for b in range(2):
        on = (gaps[b : b + 1, :] == 1) & (col[0:1] + b * BAND < counts[0])
        wm[b * BAND : (b + 1) * BAND] = jnp.broadcast_to(jnp.where(on, 1.0, 0.0), (BAND, BAND)).T

    for b in range(2):
        hq[0, 1 + b] = enc_v(wm[b * BAND : (b + 1) * BAND] * obs[b * BAND : (b + 1) * BAND])
    pl.semaphore_wait(barrier, len(peers))
    for place, goal, step in ((2, 0, t_up), (1, 3, t_down)):
        send(
            hq.at[0, place], hq.at[0, goal], sem_hs.at[0, goal], sem_hr.at[0, goal],
            z=lax.div(step, NY), y=lax.rem(step, NY),
        )
        sent(hq.at[0, place], sem_hs.at[0, goal])

    keep_first = jnp.where(t == 0, 0.0, 1.0).astype(F32)
    keep_last = jnp.where(t == NZ * NY - 1, 0.0, 1.0).astype(F32)
    rolled = pltpu.roll(jnp.broadcast_to(taps[...], (BAND, BAND)), 0, 1, stride=1, stride_axis=0)
    lot = jnp.where(col >= row, rolled, 0.0)
    upt = jnp.where(col < row, rolled, 0.0)
    ll = dot_t(lot, lot, HIGH)
    uu = dot_t(upt, upt, HIGH)
    lu = dot_t(lot, upt, HIGH)
    ul = dot_t(upt, lot, HIGH)
    zero = jnp.zeros((BAND, BAND), F32)
    bm[0:BAND, 0:BAND] = keep_first * lu
    bm[0:BAND, BAND : 2 * BAND] = ll + uu
    bm[0:BAND, 2 * BAND : 3 * BAND] = ul
    bm[0:BAND, 3 * BAND :] = zero
    bm[BAND:, 0:BAND] = zero
    bm[BAND:, BAND : 2 * BAND] = lu
    bm[BAND:, 2 * BAND : 3 * BAND] = ll + keep_last * uu
    bm[BAND:, 3 * BAND :] = keep_last * ul

    line = lax.div(t * OWN, LANES)
    shift = t * OWN - line * LANES
    for diag, part_a, part_b in ((kaula, kda, kdb), (precond, pca, pcb)):
        for k in range(3):
            values = diag[pl.ds(jnp.minimum(line + k, diag.shape[0] - 1), 1), :]
            column[k * LANES : (k + 1) * LANES] = jnp.broadcast_to(values, (LANES, LANES)).T
        row_a = lax.broadcasted_iota(I32, (RA, LANES), 0)
        row_b = lax.broadcasted_iota(I32, (RB, LANES), 0)
        part_a[...] = jnp.where(row_a < NA, column[pl.ds(shift, RA), :], 0.0)
        part_b[...] = jnp.where(row_b < NB, column[pl.ds(shift + NA, RB), :], 0.0)

    def picked(p):
        first = jnp.minimum(lax.div(p * OWN, LANES), design.shape[1] // LANES - 3)
        window = design[:, pl.ds(pl.multiple_of(first * LANES, LANES), WIDE)]
        place = lax.broadcasted_iota(I32, (2 * LANES, WIDE), 0)
        wanted = jnp.where(place < LANES, place, place - LANES + NA)
        real = ((place < NA) | (place >= LANES)) & (place < LANES + NB)
        at = lax.broadcasted_iota(I32, (2 * LANES, WIDE), 1) - (p * OWN - first * LANES)
        return window, jnp.where((at == wanted) & real, 1.0, 0.0).astype(BF16)

    def put_rows(p, carry):
        window, pick = picked(p)
        rows = dot_t(pick, window).astype(BF16)
        zz, yy = lax.div(p, NY), lax.rem(p, NY)
        ata[zz, yy] = rows[0:RA]
        atb[yy, zz] = rows[LANES : LANES + RB]
        return carry

    def put_columns(p, carry):
        window, pick = picked(p)
        columns = dot_t(window, pick).astype(BF16)
        zz, yy = lax.div(p, NY), lax.rem(p, NY)
        aa[zz, :, pl.ds(pl.multiple_of(yy * LANES, LANES), LANES)] = columns[:, 0:LANES]
        ab[yy, :, pl.ds(pl.multiple_of(zz * LANES, LANES), LANES)] = columns[:, LANES:]
        for it in range(2):
            ga[it, zz, yy, RA:] = jnp.zeros((LANES - RA, LANES), BF16)
            gb[it, yy, zz, RB:] = jnp.zeros((LANES - RB, LANES), BF16)
        return carry

    def at_a(target):
        return ata[target].reshape(NY * RA, 2 * BAND)

    def at_b(target):
        return atb[target].reshape(NZ * RB, 2 * BAND)

    lax.fori_loop(0, NZ * NY, put_rows, 0)

    def filtered(st):
        ext = dec_v(hq[st])
        w = (wm[...] * dot(bm[...], ext.reshape(4 * BAND, BAND), HIGH)).astype(BF16)
        inner = ext[1] * w[0:BAND].astype(F32) + ext[2] * w[BAND:].astype(F32)
        return w, jnp.sum(inner, 0, keepdims=True)

    def small_start(i, block):
        scs[i, 0] = block
        for k in range(1, NY):
            send(scs.at[i, 0], scr.at[i, k], sem_cs.at[i, 0], sem_cr.at[i, k], y=yp[k])

    def small_middle(i):
        sent(scr.at[i, pl.ds(0, NY - 1)], sem_cs.at[i, 0])
        total = scs[i, 0]
        for k in range(1, NY):
            arrived(scr.at[i, k], sem_cs.at[i, 0], sem_cr.at[i, k], y=yp[k])
            total = total + scr[i, k]
        scs[i, 1] = total
        for k in range(1, NZ):
            send(scs.at[i, 1], scr.at[i, NY + k], sem_cs.at[i, 1], sem_cr.at[i, NY + k], z=zp[k])

    def small_end(i):
        sent(scr.at[i, pl.ds(0, NZ - 1)], sem_cs.at[i, 1])
        total = scs[i, 1]
        for k in range(1, NZ):
            arrived(scr.at[i, NY + k], sem_cs.at[i, 1], sem_cr.at[i, NY + k], z=zp[k])
            total = total + scr[i, NY + k]
        return total

    half = NZ // 2 * RB

    def long_way(j):
        return 0 if j in (0, 3) else 1

    def hops(way, j):
        return NZ // 2 if long_way(j) == way else NZ // 2 - 1

    def scatter(st, w, early, late, fill):
        ways_y = ((0, yp[1]), (1, ym[1]))

        def send_b(way, kind, peer):
            send(sb.at[st, way, kind], rb.at[st, way, kind], sem_sb.at[st], sem_rb.at[way, kind], y=peer)

        def got_b(way, kind):
            arrived(rb.at[st, way, kind], sem_sb.at[st], sem_rb.at[way, kind], y=yp[1])

        def send_a(way, s, j):
            send(
                sa.at[st, way, s, j], ra.at[st, way, s, j], sem_sa.at[st, way, abs(long_way(j) - way)],
                sem_ra.at[way, s, j], z=zp[1] if way == 0 else zm[1],
            )

        def got_a(way, s, j):
            arrived(ra.at[st, way, s, j], sem_sa.at[st, way, 0], sem_ra.at[way, s, j], z=zp[1])

        part = dot(at_b(yp[2]), w).reshape(2, NZ // 2, RB, 128)
        for way, peer in ways_y:
            sb[st, way, 0] = enc_b(part[way])
            send_b(way, 0, peer)
        far = enc_a(dot(at_a(zp[4]), w).reshape(NY, RA, 128))
        for j in range(NY):
            sa[st, long_way(j), 0, j] = far[j]
            send_a(long_way(j), 0, j)
        for way, target in ((0, zp[3]), (1, zm[3])):
            near = dot(at_a(target), w).reshape(NY, RA, 128)
            y_a[target] = near
            for j in range(NY):
                if long_way(j) != way:
                    sa[st, way, 0, j] = enc_a(near[j])
                    send_a(way, 0, j)
        for way, peer in ways_y:
            part = dot(at_b(peer), w).reshape(2, NZ // 2, RB, 128)
            sb[st, way, 1] = enc_b(part[1 - way])
            send_b(way, 1, peer)
            y_c[way] = part[way]

        def product(i, carry):
            target = lax.rem(z + NZ - 2 + i, NZ)
            y_a[target] = dot(at_a(target), w).reshape(NY, RA, 128)
            return carry

        lax.fori_loop(0, 5, product, 0)
        y_b[...] = dot(at_b(y), w).reshape(NZ, RB, 128)
        early()
        for s in range(1, 4):
            for j in (0, 3, 1, 2):
                for way in (long_way(j), 1 - long_way(j)):
                    if s < hops(way, j):
                        got_a(way, s - 1, j)
                        target = zp[hops(way, j) - s] if way == 0 else zm[hops(way, j) - s]
                        sa[st, way, s, j] = enc_a(dec_a(ra[st, way, s - 1, j]) + y_a[target, j])
                        send_a(way, s, j)
                fill((s - 1) * NY + j)
            if s == 1:
                for way, peer in ways_y:
                    got_b(way, 0)
                    sb[st, way, 2] = enc_b(y_c[way] + dec_b(rb[st, way, 0]))
                    send_b(way, 2, peer)
                late()
            if s == 2:
                for way, peer in ways_y:
                    for kind in (1, 2):
                        got_b(way, kind)
                low = y_b[0 : NZ // 2] + dec_b(rb[st, 0, 2]) + dec_b(rb[st, 1, 1])
                y_b[0 : NZ // 2] = low
                szb[st, 0 : NZ // 2] = enc_b(low)
                high = y_b[NZ // 2 :] + dec_b(rb[st, 0, 1]) + dec_b(rb[st, 1, 2])
                y_b[NZ // 2 :] = high
                szb[st, NZ // 2 :] = enc_b(high)
                for k in (4, 3, 5, 2, 6, 1, 7):
                    send(szb.at[st, zp[k]], rzb.at[st, k], sem_szb.at[st], sem_rzb.at[k], z=zp[k])
        for j in (0, 3, 1, 2):
            for way in range(2):
                got_a(way, hops(way, j) - 1, j)
            total = dec_a(ra[st, 0, hops(0, j) - 1, j]) + dec_a(ra[st, 1, hops(1, j) - 1, j]) + y_a[z, j]
            y_a[z, j] = total
            sya[st, j] = enc_a(total)
        for k in (2, 1, 3):
            send(sya.at[st, yp[k]], rya.at[st, k], sem_sya.at[st], sem_rya.at[k], y=yp[k])
        sum_b = y_b[z]
        for k in range(1, NZ):
            arrived(rzb.at[st, k], sem_szb.at[st], sem_rzb.at[k], z=zp[k])
            sum_b = sum_b + dec_b(rzb[st, k])
        sum_a = y_a[z, y]
        for k in range(1, NY):
            arrived(rya.at[st, k], sem_sya.at[st], sem_rya.at[k], y=yp[k])
            sum_a = sum_a + dec_a(rya[st, k])
        for way in range(2):
            sent(sa.at[st, way, :, pl.ds(0, 2)], sem_sa.at[st, way, 0])
            sent(sa.at[st, way, pl.ds(0, 3), pl.ds(0, 2)], sem_sa.at[st, way, 1])
        sent(sb.at[st], sem_sb.at[st])
        sent(szb.at[st, pl.ds(0, NZ - 1)], sem_szb.at[st])
        sent(sya.at[st, pl.ds(0, NY - 1)], sem_sya.at[st])
        return sum_a, sum_b

    first_half, second_half = (0, 1, 7, 2), (6, 3, 5, 4)

    def gathered_product(it, rows_a, rows_b, middle):
        ga[it, z, y, 0:RA] = rows_a.astype(BF16)
        gb[it, y, z, 0:RB] = rows_b.astype(BF16)

        def part_a(it, zz, yy):
            return ga.at[it, zz, yy, pl.ds(0, RA)]

        def part_b(it, yy, zz):
            return gb.at[it, yy, zz, pl.ds(0, RB)]

        def put_a(way, s, k):
            block = part_a(it, zm[s] if way == 0 else zp[s], ym[k])
            send(block, block, sem_gs.at[it, 0], sem_ga.at[way, s, k], z=zp[1] if way == 0 else zm[1])

        def got_a(way, s, k):
            block = part_a(it, zm[s + 1] if way == 0 else zp[s + 1], ym[k])
            arrived(block, sem_gs.at[it, 0], sem_ga.at[way, s, k], z=zp[1])

        def put_b(way, s, k):
            block = part_b(it, ym[s] if way == 0 else yp[s], zm[k])
            send(block, block, sem_gs.at[it, 1], sem_gby.at[way, s, k], y=yp[1] if way == 0 else ym[1])

        def got_b(way, s, k):
            block = part_b(it, ym[s + 1] if way == 0 else yp[s + 1], zm[k])
            arrived(block, sem_gs.at[it, 1], sem_gby.at[way, s, k], y=yp[1])

        def from_z(k):
            arrived(part_b(it, y, zm[k]), sem_gs.at[it, 3], sem_gb.at[k], z=zp[k])
            if k == 5:
                send(part_b(it, y, zm[5]), part_b(it, y, zm[5]), sem_gs.at[it, 3], sem_gb.at[4], z=zm[1])
            put_b(0, 0, k)
            put_b(1, 0, k)

        own_a, own_b = part_a(it, z, y), part_b(it, y, z)
        for k in (2, 1, 3):
            send(own_a, own_a, sem_gs.at[it, 2], sem_gay.at[k], y=yp[k])
        put_a(0, 0, 0)
        put_a(1, 0, 0)
        for k in (5, 3, 2, 6, 1, 7):
            send(own_b, own_b, sem_gs.at[it, 3], sem_gb.at[k], z=zp[k])
        put_b(0, 0, 0)
        put_b(1, 0, 0)
        for k in (1, 3, 2):
            arrived(part_a(it, z, ym[k]), sem_gs.at[it, 2], sem_gay.at[k], y=yp[k])
            put_a(0, 0, k)
            put_a(1, 0, k)
        v = dot(aa[z], ga[it, z].reshape(NY * LANES, LANES))
        for s in range(1, 4):
            for k in (0, 1, 3, 2):
                for way in (long_way(k), 1 - long_way(k)):
                    got_a(way, s - 1, k)
                    if s < hops(way, k):
                        put_a(way, s, k)
            if s == 1:
                for k in (1, 7, 2, 6, 5, 3):
                    from_z(k)
            if s == 2:
                from_z(4)
                for k in first_half:
                    got_b(0, 0, k)
                    put_b(0, 1, k)
                for k in second_half:
                    got_b(1, 0, k)
                    put_b(1, 1, k)
                middle()
            v = v + dot(aa[zm[s]], ga[it, zm[s]].reshape(NY * LANES, LANES))
            v = v + dot(aa[zp[s]], ga[it, zp[s]].reshape(NY * LANES, LANES))
        v = v + dot(ab[y], gb[it, y].reshape(NZ * LANES, LANES))
        for k in second_half:
            got_b(0, 0, k)
        for k in first_half:
            got_b(1, 0, k)
        v = v + dot(ab[yp[1]], gb[it, yp[1]].reshape(NZ * LANES, LANES))
        v = v + dot(ab[ym[1]], gb[it, ym[1]].reshape(NZ * LANES, LANES))
        for k in first_half:
            got_b(0, 1, k)
        for k in second_half:
            got_b(1, 1, k)
        v = v + dot(ab[yp[2]], gb[it, yp[2]].reshape(NZ * LANES, LANES))
        for k in range(NY):
            got_a(long_way(k), 3, k)
        sent(ga.at[it, pl.ds(0, NZ - 1), :, pl.ds(0, RA)], sem_gs.at[it, 0])
        sent(gb.at[it, pl.ds(0, NY - 1), :, pl.ds(0, RB)], sem_gs.at[it, 1])
        sent(ga.at[it, 0, pl.ds(0, NY - 1), pl.ds(0, RA)], sem_gs.at[it, 2])
        sent(gb.at[it, 0, pl.ds(0, NZ - 1), pl.ds(0, RB)], sem_gs.at[it, 3])
        return v + dot(aa[zm[4]], ga[it, zm[4]].reshape(NY * LANES, LANES))

    def slab_values(it, v, scal, finish):
        vs[it] = v.reshape(2, BAND, 128)
        scc[it, 0] = scal
        send(vs.at[it, other], vr.at[it], sem_vs.at[it, 0], sem_vr.at[it, 0], c=other)
        send(scc.at[it, 0], scc.at[it, 1], sem_vs.at[it, 1], sem_vr.at[it, 1], c=other)
        arrived(vr.at[it], sem_vs.at[it, 0], sem_vr.at[it, 0], c=other)
        chip = vs[it, c] + vr[it]
        us[it] = enc_v(chip)
        for k in (2, 1, 3):
            send(us.at[it], ur.at[it, k], sem_us.at[it, 0], sem_ur.at[it, k], x=xp[k])
        arrived(scc.at[it, 1], sem_vs.at[it, 1], sem_vr.at[it, 1], c=other)
        scal = scc[it, 0] + scc[it, 1]
        scx[it, 0] = scal
        for k in (2, 1, 3):
            send(scx.at[it, 0], scx.at[it, k], sem_us.at[it, 1], sem_uc.at[it, k], x=xp[k])
        for k in range(1, NX):
            arrived(ur.at[it, k], sem_us.at[it, 0], sem_ur.at[it, k], x=xp[k])
            chip = chip + dec_v(ur[it, k])
            arrived(scx.at[it, k], sem_us.at[it, 1], sem_uc.at[it, k], x=xp[k])
            scal = scal + scx[it, k]
        mask = wm[pl.ds(pl.multiple_of(c * BAND, BAND), BAND), :]
        block, scal = finish(mask * chip, scal)
        hq[it + 1, 1 + c] = enc_v(block)
        slot = 3 - 3 * c
        step = jnp.where(c == 0, t_down, t_up)
        mine = hq.at[it + 1, 1 + c]
        for core in range(NC):
            send(
                mine, hq.at[it + 1, slot], sem_hs.at[it + 1, 1 + core], sem_hr.at[it + 1, slot],
                z=lax.div(step, NY), y=lax.rem(step, NY), c=jnp.int32(core),
            )
        send(mine, mine, sem_hs.at[it + 1, 0], sem_hr.at[it + 1, 1 + c], c=other)
        for k in range(3):
            sent(mine, sem_hs.at[it + 1, k])
        sent(vs.at[it, 0], sem_vs.at[it, 0])
        sent(scc.at[it, 0], sem_vs.at[it, 1])
        sent(ur.at[it, pl.ds(0, NX - 1)], sem_us.at[it, 0])
        sent(scx.at[it, pl.ds(0, NX - 1)], sem_us.at[it, 1])
        for place in (2 - c, 0, 3):
            arrived(hq.at[it + 1, place], sem_hs.at[it + 1, 0], sem_hr.at[it + 1, place], c=other)
        return block, scal

    arrived(hq.at[0, 0], sem_hs.at[0, 0], sem_hr.at[0, 0], c=other)
    arrived(hq.at[0, 3], sem_hs.at[0, 0], sem_hr.at[0, 3], c=other)

    def nothing(*_):
        return None

    def some_columns(i):
        lax.fori_loop(3 * i, min(3 * i + 3, NZ * NY), put_columns, 0)

    w, _ = filtered(0)
    res_a, res_b = scatter(0, w, nothing, nothing, some_columns)

    def col_sum(a, b):
        return jnp.sum(a, 0, keepdims=True) + jnp.sum(b, 0, keepdims=True)

    def rows_of(*rows):
        spare = jnp.zeros((8 - len(rows), 128), F32)
        return jnp.concatenate([*rows, spare], 0)

    dir_a, dir_b = pca[...] * res_a, pcb[...] * res_b
    small_start(0, rows_of(col_sum(res_a * dir_a, res_b * dir_b), col_sum(kda[...] * dir_a * dir_a, kdb[...] * dir_b * dir_b)))
    v = gathered_product(0, dir_a, dir_b, lambda: small_middle(0))
    block, scal = slab_values(0, v, small_end(0), lambda block, scal: (block, scal))
    norm, diag = scal[0:1], scal[1:2]

    w, inner = filtered(1)
    image_a, image_b = scatter(1, w, lambda: small_start(1, rows_of(inner)), lambda: small_middle(1), nothing)
    step_len = norm / (diag + small_end(1)[0:1])
    image_a, image_b = image_a + kda[...] * dir_a, image_b + kdb[...] * dir_b
    sol_a, sol_b = step_len * dir_a, step_len * dir_b
    res_a, res_b = res_a - step_len * image_a, res_b - step_len * image_b
    scaled_a, scaled_b = pca[...] * res_a, pcb[...] * res_b
    small_start(
        2,
        rows_of(
            col_sum(res_a * scaled_a, res_b * scaled_b),
            col_sum(kda[...] * scaled_a * scaled_a, kdb[...] * scaled_b * scaled_b),
            col_sum(kda[...] * scaled_a * dir_a, kdb[...] * scaled_b * dir_b),
        ),
    )
    v = gathered_product(1, scaled_a, scaled_b, lambda: small_middle(2))

    def finish(new_block, scal):
        ratio = scal[0:1] / norm
        return new_block + ratio * block, scal

    _, scal = slab_values(1, v, small_end(2), finish)
    ratio = scal[0:1] / norm
    norm = scal[0:1]
    diag = scal[1:2] + 2.0 * ratio * scal[2:3] + ratio * ratio * diag
    dir_a, dir_b = scaled_a + ratio * dir_a, scaled_b + ratio * dir_b
    w, last_inner = filtered(2)
    image_a, image_b = scatter(2, w, lambda: small_start(3, rows_of(last_inner)), lambda: small_middle(3), nothing)
    step_len = norm / (diag + small_end(3)[0:1])
    image_a, image_b = image_a + kda[...] * dir_a, image_b + kdb[...] * dir_b
    sol_a, sol_b = sol_a + step_len * dir_a, sol_b + step_len * dir_b
    res_a, res_b = res_a - step_len * image_a, res_b - step_len * image_b
    xout[0:NA] = sol_a[0:NA]
    xout[NA:] = sol_b[0:NB]
    rout[0:NA] = res_a[0:NA]
    rout[NA:] = res_b[0:NB]
    for copy in pending:
        copy.wait_send()


def shards(design, observed, slab_counts, gap_mask, filter_taps, kaula_diag, precond):
    rows = observed.shape[0]
    coefs = design.shape[1]
    dma = pltpu.SemaphoreType.DMA
    args = (
        design, observed, slab_counts, gap_mask.reshape(rows // LANES, LANES), filter_taps.reshape(1, LANES),
        kaula_diag.reshape(coefs // LANES, LANES), precond.reshape(coefs // LANES, LANES),
    )
    vm = pltpu.VMEM
    scratch = [
        vm((NZ, rows, NY * LANES), BF16),
        vm((NY, rows, NZ * LANES), BF16),
        vm((NZ, NY, RA, rows), BF16),
        vm((NY, NZ, RB, rows), BF16),
        vm((rows, LANES), F32),
        vm((RA, LANES), F32), vm((RB, LANES), F32), vm((RA, LANES), F32), vm((RB, LANES), F32),
        vm((4 * LANES, LANES), F32),
        vm((2 * BAND, 4 * BAND), F32),
        vm((NZ, NY, RA, 128), F32),
        vm((NZ, RB, 128), F32),
        vm((2, NZ // 2, RB, 128), F32),
        vm((3, 2, 4, NY, RA, 128), I16),
        vm((3, 2, 4, NY, RA, 128), I16),
        vm((3, NY, RA, 128), I16),
        vm((3, NY, RA, 128), I16),
        vm((3, 2, 3, NZ // 2, RB, 128), I16),
        vm((3, 2, 3, NZ // 2, RB, 128), I16),
        vm((3, NZ, RB, 128), I16),
        vm((3, NZ, RB, 128), I16),
        vm((2, NZ, NY, LANES, LANES), BF16),
        vm((2, NY, NZ, LANES, LANES), BF16),
        vm((2, 2, BAND, 128), F32),
        vm((2, BAND, 128), F32),
        vm((2, BAND + 16, 128), I16),
        vm((2, NX, BAND + 16, 128), I16),
        vm((3, 4, BAND + 16, 128), I16),
        vm((4, 2, 8, 128), F32),
        vm((4, NY + NZ, 8, 128), F32),
        vm((2, 2, 8, 128), F32),
        vm((2, NX, 8, 128), F32),
        dma((3, 2, 2)), dma((2, 4, NY)), dma((3,)), dma((NY,)),
        dma((3,)), dma((2, 3)), dma((3,)), dma((NZ,)),
        dma((2, 4)), dma((2, 4, NY)), dma((NY,)), dma((NZ,)), dma((2, 2, NZ)),
        dma((2, 2)), dma((2, 2)), dma((2, 2)), dma((2, NX)), dma((2, NX)), dma((3, 4)), dma((3, 4)),
        dma((4, 2)), dma((4, NY + NZ)),
    ]
    out = jax.ShapeDtypeStruct((OWN, LANES), F32)
    return pl.pallas_call(
        kernel,
        name="cg",
        out_shape=(out, out),
        in_specs=[pl.BlockSpec(memory_space=pltpu.SMEM if i == 2 else vm) for i in range(len(args))],
        out_specs=(pl.BlockSpec(memory_space=vm),) * 2,
        scratch_shapes=scratch,
        compiler_params=pltpu.CompilerParams(
            collective_id=0, has_side_effects=True, vmem_limit_bytes=60 * 1024 * 1024
        ),
    )(*args)


def solution(mesh):
    torus = Mesh(mesh.devices.reshape(NZ, NY, NX, NC), AXES)
    in_specs = (P(TM, COEF), P(TM, None), P(TM), P(TM), P(), P(COEF), P(COEF))
    out_specs = (P((*COEF, *TM), None),) * 2
    return jax.shard_map(shards, mesh=torus, in_specs=in_specs, out_specs=out_specs, check_vma=False)
```

```python
import functools

import jax
import jax.numpy as jnp
from jax import lax
from jax.experimental import pallas as pl
from jax.experimental.pallas import tpu as pltpu
from jax.sharding import Mesh
from jax.sharding import PartitionSpec as P

AXES = ("z", "y", "x", "c")
TM = ("z", "y")
COEF = ("x", "c")
MESH = pl.DeviceIdType.MESH
NZ, NY, NX, NC = 8, 4, 4, 2
NA, NB = 104, 92
RA, RB = 112, 96
OWN = NA + NB
LANES = 128
WIDE = 3 * LANES
I16 = jnp.int16
I32 = jnp.int32
BAND = 128
F32 = jnp.float32
BF16 = jnp.bfloat16
HIGH = lax.Precision.HIGHEST


def dot(a, b, precision=None):
    return jnp.dot(a, b, preferred_element_type=F32, precision=precision)


def dot_t(a, b, precision=None):
    return lax.dot_general(a, b, (((1,), (1,)), ((), ())), preferred_element_type=F32, precision=precision)


def split(v):
    high = v.astype(BF16)
    return high, (v - high.astype(F32)).astype(BF16)


HEADROOM = 0.998


def encoded(v, spare):
    tail = v.shape[-2] - 8
    top = jnp.maximum(jnp.max(jnp.abs(v), axis=-2, keepdims=True), 1e-30)
    power = jnp.floor(jnp.log2(top)) + 1.0
    q = jnp.round(v * (jnp.exp2(15.0 - power) * HEADROOM))
    row = lax.broadcasted_iota(I32, (*v.shape[:-2], 8, v.shape[-1]), v.ndim - 2)
    last = jnp.where(row == spare - tail, power, q[..., tail:, :])
    return jnp.concatenate([q[..., :tail, :], last], -2).astype(I32).astype(I16)


def decoded(q, spare):
    v = q.astype(I32).astype(F32)
    return v * (jnp.exp2(v[..., spare : spare + 1, :] - 15.0) * (1.0 / HEADROOM))


def enc_a(v):
    return encoded(v, NA)


def enc_b(v):
    return encoded(v, NB)


def dec_a(q):
    return decoded(q, NA)


def dec_b(q):
    return decoded(q, NB)


def enc_v(v):
    return encoded(jnp.concatenate([v, jnp.zeros((16, LANES), F32)], 0), BAND + 8)


def dec_v(q):
    return decoded(q, BAND + 8)[..., 0:BAND, :]


def rcopy(src, dst, ssem, rsem, **device):
    return pltpu.make_async_remote_copy(
        src_ref=src, dst_ref=dst, send_sem=ssem, recv_sem=rsem, device_id=device, device_id_type=MESH
    )


def kernel(
    design, obs, counts, gaps, taps, kaula, precond,
    xout, rout,
    aa, ab, ata, atb, wm, kda, kdb, pca, pcb, column, bm, bm_high, bm_low, y_a, y_b, y_c,
    sa, ra, sya, rya, sb, rb, szb, rzb,
    ga, gb, vs, vr, us, ur, hq, scs, scr, scc, scx,
    sem_sa, sem_ra, sem_sya, sem_rya, sem_sb, sem_rb, sem_szb, sem_rzb,
    sem_gs, sem_ga, sem_gay, sem_gb, sem_gby,
    sem_vs, sem_vr, sem_us, sem_ur, sem_uc, sem_hs, sem_hr, sem_cs, sem_cr,
):
    z, y, x, c = (lax.axis_index(name) for name in AXES)
    t = z * NY + y
    zp = [lax.rem(z + k, NZ) for k in range(NZ)]
    zm = [lax.rem(z + NZ - k, NZ) for k in range(NZ)]
    yp = [lax.rem(y + k, NY) for k in range(NY)]
    ym = [lax.rem(y + NY - k, NY) for k in range(NY)]
    xp = [lax.rem(x + k, NX) for k in range(NX)]
    other = 1 - c
    t_up = lax.rem(t + 1, NZ * NY)
    t_down = lax.rem(t + NZ * NY - 1, NZ * NY)
    pending = []

    def send(src, dst, ssem, rsem, **device):
        rcopy(src, dst, ssem, rsem, **device).start()

    def sent(ref, sem):
        pending.append(rcopy(ref, ref, sem, sem, c=other))

    def arrived(dst, ssem, rsem, **device):
        rcopy(dst, dst, ssem, rsem, **device).wait_recv()

    barrier = pltpu.get_barrier_semaphore()
    peers = [dict(z=zp[k]) for k in range(1, NZ)] + [dict(y=yp[k]) for k in range(1, NY)]
    peers += [dict(x=xp[k]) for k in range(1, NX)] + [dict(c=other)]
    for step in (t_up, t_down):
        for core in range(NC):
            peers.append(dict(z=lax.div(step, NY), y=lax.rem(step, NY), c=jnp.int32(core)))
    for peer in peers:
        pl.semaphore_signal(barrier, inc=1, device_id=peer, device_id_type=MESH)

    row = lax.broadcasted_iota(I32, (BAND, BAND), 0)
    col = lax.broadcasted_iota(I32, (BAND, BAND), 1)
    for b in range(2):
        on = (gaps[b : b + 1, :] == 1) & (col[0:1] + b * BAND < counts[0])
        wm[b * BAND : (b + 1) * BAND] = jnp.broadcast_to(jnp.where(on, 1.0, 0.0), (BAND, BAND)).T

    for b in range(2):
        hq[0, 1 + b] = enc_v(wm[b * BAND : (b + 1) * BAND] * obs[b * BAND : (b + 1) * BAND])
    def picked(p):
        first = jnp.minimum(lax.div(p * OWN, LANES), design.shape[1] // LANES - 3)
        window = design[:, pl.ds(pl.multiple_of(first * LANES, LANES), WIDE)]
        place = lax.broadcasted_iota(I32, (2 * LANES, WIDE), 0)
        wanted = jnp.where(place < LANES, place, place - LANES + NA)
        real = ((place < NA) | (place >= LANES)) & (place < LANES + NB)
        at = lax.broadcasted_iota(I32, (2 * LANES, WIDE), 1) - (p * OWN - first * LANES)
        return window, jnp.where((at == wanted) & real, 1.0, 0.0).astype(BF16)

    def put_rows(p, carry):
        window, pick = picked(p)
        rows = dot_t(pick, window).astype(BF16)
        zz, yy = lax.div(p, NY), lax.rem(p, NY)
        ata[zz, yy] = rows[0:RA]
        atb[yy, zz] = rows[LANES : LANES + RB]
        return carry

    def put_columns(p, carry):
        window, pick = picked(p)
        columns = dot_t(window, pick).astype(BF16)
        zz, yy = lax.div(p, NY), lax.rem(p, NY)
        aa[zz, :, pl.ds(pl.multiple_of(yy * LANES, LANES), LANES)] = columns[:, 0:LANES]
        ab[yy, :, pl.ds(pl.multiple_of(zz * LANES, LANES), LANES)] = columns[:, LANES:]
        for it in range(2):
            ga[it, zz, yy, RA:] = jnp.zeros((LANES - RA, LANES), BF16)
            gb[it, yy, zz, RB:] = jnp.zeros((LANES - RB, LANES), BF16)
        return carry

    def at_a(target):
        return ata[target].reshape(NY * RA, 2 * BAND)

    def at_b(target):
        return atb[target].reshape(NZ * RB, 2 * BAND)

    early_rows = 16
    lax.fori_loop(0, early_rows, put_rows, 0)
    pl.semaphore_wait(barrier, len(peers))
    for place, goal, step in ((2, 0, t_up), (1, 3, t_down)):
        send(
            hq.at[0, place], hq.at[0, goal], sem_hs.at[0, goal], sem_hr.at[0, goal],
            z=lax.div(step, NY), y=lax.rem(step, NY),
        )
        sent(hq.at[0, place], sem_hs.at[0, goal])

    keep_first = jnp.where(t == 0, 0.0, 1.0).astype(F32)
    keep_last = jnp.where(t == NZ * NY - 1, 0.0, 1.0).astype(F32)
    rolled = pltpu.roll(jnp.broadcast_to(taps[...], (BAND, BAND)), 0, 1, stride=1, stride_axis=0)
    lot = jnp.where(col >= row, rolled, 0.0)
    upt = jnp.where(col < row, rolled, 0.0)
    ll = dot_t(lot, lot, HIGH)
    uu = dot_t(upt, upt, HIGH)
    lu = dot_t(lot, upt, HIGH)
    ul = dot_t(upt, lot, HIGH)
    zero = jnp.zeros((BAND, BAND), F32)
    bm[0:BAND, 0:BAND] = keep_first * lu
    bm[0:BAND, BAND : 2 * BAND] = ll + uu
    bm[0:BAND, 2 * BAND : 3 * BAND] = ul
    bm[0:BAND, 3 * BAND :] = zero
    bm[BAND:, 0:BAND] = zero
    bm[BAND:, BAND : 2 * BAND] = lu
    bm[BAND:, 2 * BAND : 3 * BAND] = ll + keep_last * uu
    bm[BAND:, 3 * BAND :] = keep_last * ul
    bm_high[...], bm_low[...] = split(bm[...])

    line = lax.div(t * OWN, LANES)
    shift = t * OWN - line * LANES
    for diag, part_a, part_b in ((kaula, kda, kdb), (precond, pca, pcb)):
        for k in range(3):
            values = diag[pl.ds(jnp.minimum(line + k, diag.shape[0] - 1), 1), :]
            column[k * LANES : (k + 1) * LANES] = jnp.broadcast_to(values, (LANES, LANES)).T
        row_a = lax.broadcasted_iota(I32, (RA, LANES), 0)
        row_b = lax.broadcasted_iota(I32, (RB, LANES), 0)
        part_a[...] = jnp.where(row_a < NA, column[pl.ds(shift, RA), :], 0.0)
        part_b[...] = jnp.where(row_b < NB, column[pl.ds(shift + NA, RB), :], 0.0)

    lax.fori_loop(early_rows, NZ * NY, put_rows, 0)

    def filtered(st):
        ext = dec_v(hq[st])
        high, low = split(ext.reshape(4 * BAND, BAND))
        series = dot(bm_high[...], high) + (dot(bm_high[...], low) + dot(bm_low[...], high))
        w = (wm[...] * series).astype(BF16)
        inner = ext[1] * w[0:BAND].astype(F32) + ext[2] * w[BAND:].astype(F32)
        return w, jnp.sum(inner, 0, keepdims=True)

    def small_start(i, block):
        scs[i, 0] = block
        for k in range(1, NY):
            send(scs.at[i, 0], scr.at[i, k], sem_cs.at[i, 0], sem_cr.at[i, k], y=yp[k])

    def small_middle(i):
        sent(scr.at[i, pl.ds(0, NY - 1)], sem_cs.at[i, 0])
        total = scs[i, 0]
        for k in range(1, NY):
            arrived(scr.at[i, k], sem_cs.at[i, 0], sem_cr.at[i, k], y=yp[k])
            total = total + scr[i, k]
        scs[i, 1] = total
        for k in range(1, NZ):
            send(scs.at[i, 1], scr.at[i, NY + k], sem_cs.at[i, 1], sem_cr.at[i, NY + k], z=zp[k])

    def small_end(i):
        sent(scr.at[i, pl.ds(0, NZ - 1)], sem_cs.at[i, 1])
        total = scs[i, 1]
        for k in range(1, NZ):
            arrived(scr.at[i, NY + k], sem_cs.at[i, 1], sem_cr.at[i, NY + k], z=zp[k])
            total = total + scr[i, NY + k]
        return total

    half = NZ // 2 * RB

    def long_way(j):
        return 0 if j in (0, 3) else 1

    def along_z(way, links):
        return zp[links] if way == 0 else zm[links]

    def scatter(st, w, early, late, fill):
        ways_y = ((0, yp[1]), (1, ym[1]))

        def send_b(way, kind, peer):
            send(sb.at[st, way, kind], rb.at[st, way, kind], sem_sb.at[st], sem_rb.at[way, kind], y=peer)

        def got_b(way, kind):
            arrived(rb.at[st, way, kind], sem_sb.at[st], sem_rb.at[way, kind], y=yp[1])

        def send_a(way, s, j):
            send(
                sa.at[st, way, s, j], ra.at[st, way, s, j], sem_sa.at[st, way, abs(long_way(j) - way)],
                sem_ra.at[way, s, j], z=along_z(way, 2 if s == 0 else 1),
            )

        def got_a(way, s, j):
            arrived(ra.at[st, way, s, j], sem_sa.at[st, way, 0], sem_ra.at[way, s, j], z=zp[1])

        part = dot(at_b(yp[2]), w).reshape(2, NZ // 2, RB, 128)
        for way, peer in ways_y:
            sb[st, way, 0] = enc_b(part[way])
            send_b(way, 0, peer)
        far = enc_a(dot(at_a(zp[4]), w).reshape(NY, RA, 128))
        for j in range(NY):
            sa[st, long_way(j), 0, j] = far[j]
            send_a(long_way(j), 0, j)
        for way in range(2):
            sa[st, way, 1] = enc_a(dot(at_a(along_z(way, 3)), w).reshape(NY, RA, 128))
            for j in range(NY):
                send_a(way, 1, j)
        for way, peer in ways_y:
            part = dot(at_b(peer), w).reshape(2, NZ // 2, RB, 128)
            sb[st, way, 1] = enc_b(part[1 - way])
            send_b(way, 1, peer)
            y_c[way] = part[way]

        def product(i, carry):
            target = lax.rem(z + NZ - 2 + i, NZ)
            y_a[target] = dot(at_a(target), w).reshape(NY, RA, 128)
            return carry

        lax.fori_loop(0, 5, product, 0)
        y_b[...] = dot(at_b(y), w).reshape(NZ, RB, 128)
        early()
        for i in range(3):
            fill(i)

        def pass_on(s, j):
            codes = []
            for way in range(2):
                got_a(way, s - 1, j)
                if s == 2 and way == long_way(j):
                    got_a(way, 0, j)
            for way in range(2):
                total = dec_a(ra[st, way, s - 1, j]) + y_a[along_z(way, 4 - s), j]
                if s == 2 and way == long_way(j):
                    total = total + dec_a(ra[st, way, 0, j])
                codes.append(enc_a(total))
            for way in range(2):
                sa[st, way, s, j] = codes[way]
            for way in range(2):
                send_a(way, s, j)

        for j in range(NY):
            pass_on(2, j)
        for way, peer in ways_y:
            got_b(way, 0)
            sb[st, way, 2] = enc_b(y_c[way] + dec_b(rb[st, way, 0]))
            send_b(way, 2, peer)
        fill(3)
        for j in range(NY):
            pass_on(3, j)
            fill(4 + j)
        late()
        for i in range(8, 11):
            fill(i)
        for way in range(2):
            for kind in (1, 2):
                got_b(way, kind)
        low = y_b[0 : NZ // 2] + dec_b(rb[st, 0, 2]) + dec_b(rb[st, 1, 1])
        y_b[0 : NZ // 2] = low
        szb[st, 0 : NZ // 2] = enc_b(low)
        high = y_b[NZ // 2 :] + dec_b(rb[st, 0, 1]) + dec_b(rb[st, 1, 2])
        y_b[NZ // 2 :] = high
        szb[st, NZ // 2 :] = enc_b(high)
        for k in (4, 3, 5, 2, 6, 1, 7):
            send(szb.at[st, zp[k]], rzb.at[st, k], sem_szb.at[st], sem_rzb.at[k], z=zp[k])
        for j in range(NY):
            for way in range(2):
                got_a(way, 3, j)
            total = dec_a(ra[st, 0, 3, j]) + dec_a(ra[st, 1, 3, j]) + y_a[z, j]
            y_a[z, j] = total
            sya[st, j] = enc_a(total)
        for k in (2, 1, 3):
            send(sya.at[st, yp[k]], rya.at[st, k], sem_sya.at[st], sem_rya.at[k], y=yp[k])
        sum_b = y_b[z]
        for k in range(1, NZ):
            arrived(rzb.at[st, k], sem_szb.at[st], sem_rzb.at[k], z=zp[k])
            sum_b = sum_b + dec_b(rzb[st, k])
        sum_a = y_a[z, y]
        for k in range(1, NY):
            arrived(rya.at[st, k], sem_sya.at[st], sem_rya.at[k], y=yp[k])
            sum_a = sum_a + dec_a(rya[st, k])
        for way in range(2):
            sent(sa.at[st, way, :, pl.ds(0, 2)], sem_sa.at[st, way, 0])
            sent(sa.at[st, way, pl.ds(0, 3), pl.ds(0, 2)], sem_sa.at[st, way, 1])
        sent(sb.at[st], sem_sb.at[st])
        sent(szb.at[st, pl.ds(0, NZ - 1)], sem_szb.at[st])
        sent(sya.at[st, pl.ds(0, NY - 1)], sem_sya.at[st])
        return sum_a, sum_b

    first_half, second_half = (0, 1, 7, 2), (6, 3, 5, 4)

    def gathered_product(it, rows_a, rows_b, middle):
        ga[it, z, y, 0:RA] = rows_a.astype(BF16)
        gb[it, y, z, 0:RB] = rows_b.astype(BF16)

        def part_a(it, zz, yy):
            return ga.at[it, zz, yy, pl.ds(0, RA)]

        def part_b(it, yy, zz):
            return gb.at[it, yy, zz, pl.ds(0, RB)]

        def put_a(way, s, k):
            block = part_a(it, along_z(1 - way, s - 1 if s else 2), ym[k])
            send(block, block, sem_gs.at[it, 0], sem_ga.at[way, s, k], z=along_z(way, 1 if s else 2))

        def got_a(way, s, k):
            block = part_a(it, along_z(1 - way, s if s else 4), ym[k])
            arrived(block, sem_gs.at[it, 0], sem_ga.at[way, s, k], z=zp[1])

        def put_b(way, s, k):
            block = part_b(it, ym[s] if way == 0 else yp[s], zm[k])
            send(block, block, sem_gs.at[it, 1], sem_gby.at[way, s, k], y=yp[1] if way == 0 else ym[1])

        def got_b(way, s, k):
            block = part_b(it, ym[s + 1] if way == 0 else yp[s + 1], zm[k])
            arrived(block, sem_gs.at[it, 1], sem_gby.at[way, s, k], y=yp[1])

        def from_z(k):
            arrived(part_b(it, y, zm[k]), sem_gs.at[it, 3], sem_gb.at[k], z=zp[k])
            if k == 5:
                send(part_b(it, y, zm[5]), part_b(it, y, zm[5]), sem_gs.at[it, 3], sem_gb.at[4], z=zm[1])
            put_b(0, 0, k)
            put_b(1, 0, k)

        own_a, own_b = part_a(it, z, y), part_b(it, y, z)
        for k in (2, 1, 3):
            send(own_a, own_a, sem_gs.at[it, 2], sem_gay.at[k], y=yp[k])
        put_a(0, 1, 0)
        put_a(1, 1, 0)
        for k in (5, 3, 2, 6, 1, 7):
            send(own_b, own_b, sem_gs.at[it, 3], sem_gb.at[k], z=zp[k])
        put_b(0, 0, 0)
        put_b(1, 0, 0)
        for k in (1, 3, 2):
            arrived(part_a(it, z, ym[k]), sem_gs.at[it, 2], sem_gay.at[k], y=yp[k])
            put_a(0, 1, k)
            put_a(1, 1, k)
        v = dot(aa[z], ga[it, z].reshape(NY * LANES, LANES))
        for s in range(1, 4):
            for k in (0, 1, 3, 2):
                for way in range(2):
                    got_a(way, s, k)
                    if s == 2 and way == long_way(k):
                        put_a(way, 0, k)
                    if s < 3:
                        put_a(way, s + 1, k)
            if s == 1:
                for k in (1, 7, 2, 6, 5, 3):
                    from_z(k)
            if s == 2:
                from_z(4)
                for k in first_half:
                    got_b(0, 0, k)
                    put_b(0, 1, k)
                for k in second_half:
                    got_b(1, 0, k)
                    put_b(1, 1, k)
                middle()
            v = v + dot(aa[zm[s]], ga[it, zm[s]].reshape(NY * LANES, LANES))
            v = v + dot(aa[zp[s]], ga[it, zp[s]].reshape(NY * LANES, LANES))
        v = v + dot(ab[y], gb[it, y].reshape(NZ * LANES, LANES))
        for k in second_half:
            got_b(0, 0, k)
        for k in first_half:
            got_b(1, 0, k)
        v = v + dot(ab[yp[1]], gb[it, yp[1]].reshape(NZ * LANES, LANES))
        v = v + dot(ab[ym[1]], gb[it, ym[1]].reshape(NZ * LANES, LANES))
        for k in first_half:
            got_b(0, 1, k)
        for k in second_half:
            got_b(1, 1, k)
        v = v + dot(ab[yp[2]], gb[it, yp[2]].reshape(NZ * LANES, LANES))
        for k in range(NY):
            got_a(long_way(k), 0, k)
        sent(ga.at[it, pl.ds(0, NZ - 1), :, pl.ds(0, RA)], sem_gs.at[it, 0])
        sent(gb.at[it, pl.ds(0, NY - 1), :, pl.ds(0, RB)], sem_gs.at[it, 1])
        sent(ga.at[it, 0, pl.ds(0, NY - 1), pl.ds(0, RA)], sem_gs.at[it, 2])
        sent(gb.at[it, 0, pl.ds(0, NZ - 1), pl.ds(0, RB)], sem_gs.at[it, 3])
        return v + dot(aa[zm[4]], ga[it, zm[4]].reshape(NY * LANES, LANES))

    def slab_values(it, v, scal, finish):
        vs[it] = v.reshape(2, BAND, 128)
        scc[it, 0] = scal
        send(vs.at[it, other], vr.at[it], sem_vs.at[it, 0], sem_vr.at[it, 0], c=other)
        send(scc.at[it, 0], scc.at[it, 1], sem_vs.at[it, 1], sem_vr.at[it, 1], c=other)
        arrived(vr.at[it], sem_vs.at[it, 0], sem_vr.at[it, 0], c=other)
        chip = vs[it, c] + vr[it]
        us[it] = enc_v(chip)
        for k in (2, 1, 3):
            send(us.at[it], ur.at[it, k], sem_us.at[it, 0], sem_ur.at[it, k], x=xp[k])
        arrived(scc.at[it, 1], sem_vs.at[it, 1], sem_vr.at[it, 1], c=other)
        scal = scc[it, 0] + scc[it, 1]
        scx[it, 0] = scal
        for k in (2, 1, 3):
            send(scx.at[it, 0], scx.at[it, k], sem_us.at[it, 1], sem_uc.at[it, k], x=xp[k])
        for k in range(1, NX):
            arrived(ur.at[it, k], sem_us.at[it, 0], sem_ur.at[it, k], x=xp[k])
            chip = chip + dec_v(ur[it, k])
            arrived(scx.at[it, k], sem_us.at[it, 1], sem_uc.at[it, k], x=xp[k])
            scal = scal + scx[it, k]
        mask = wm[pl.ds(pl.multiple_of(c * BAND, BAND), BAND), :]
        block, scal = finish(mask * chip, scal)
        hq[it + 1, 1 + c] = enc_v(block)
        slot = 3 - 3 * c
        step = jnp.where(c == 0, t_down, t_up)
        mine = hq.at[it + 1, 1 + c]
        for core in range(NC):
            send(
                mine, hq.at[it + 1, slot], sem_hs.at[it + 1, 1 + core], sem_hr.at[it + 1, slot],
                z=lax.div(step, NY), y=lax.rem(step, NY), c=jnp.int32(core),
            )
        send(mine, mine, sem_hs.at[it + 1, 0], sem_hr.at[it + 1, 1 + c], c=other)
        for k in range(3):
            sent(mine, sem_hs.at[it + 1, k])
        sent(vs.at[it, 0], sem_vs.at[it, 0])
        sent(scc.at[it, 0], sem_vs.at[it, 1])
        sent(ur.at[it, pl.ds(0, NX - 1)], sem_us.at[it, 0])
        sent(scx.at[it, pl.ds(0, NX - 1)], sem_us.at[it, 1])
        for place in (2 - c, 0, 3):
            arrived(hq.at[it + 1, place], sem_hs.at[it + 1, 0], sem_hr.at[it + 1, place], c=other)
        return block, scal

    arrived(hq.at[0, 0], sem_hs.at[0, 0], sem_hr.at[0, 0], c=other)
    arrived(hq.at[0, 3], sem_hs.at[0, 0], sem_hr.at[0, 3], c=other)

    def nothing(*_):
        return None

    def some_columns(i):
        lax.fori_loop(3 * i, min(3 * i + 3, NZ * NY), put_columns, 0)

    w, _ = filtered(0)
    res_a, res_b = scatter(0, w, nothing, nothing, some_columns)

    def col_sum(a, b):
        return jnp.sum(a, 0, keepdims=True) + jnp.sum(b, 0, keepdims=True)

    def rows_of(*rows):
        spare = jnp.zeros((8 - len(rows), 128), F32)
        return jnp.concatenate([*rows, spare], 0)

    dir_a, dir_b = pca[...] * res_a, pcb[...] * res_b
    small_start(0, rows_of(col_sum(res_a * dir_a, res_b * dir_b), col_sum(kda[...] * dir_a * dir_a, kdb[...] * dir_b * dir_b)))
    v = gathered_product(0, dir_a, dir_b, lambda: small_middle(0))
    block, scal = slab_values(0, v, small_end(0), lambda block, scal: (block, scal))
    norm, diag = scal[0:1], scal[1:2]

    w, inner = filtered(1)
    image_a, image_b = scatter(1, w, lambda: small_start(1, rows_of(inner)), lambda: small_middle(1), nothing)
    step_len = norm / (diag + small_end(1)[0:1])
    image_a, image_b = image_a + kda[...] * dir_a, image_b + kdb[...] * dir_b
    sol_a, sol_b = step_len * dir_a, step_len * dir_b
    res_a, res_b = res_a - step_len * image_a, res_b - step_len * image_b
    scaled_a, scaled_b = pca[...] * res_a, pcb[...] * res_b
    small_start(
        2,
        rows_of(
            col_sum(res_a * scaled_a, res_b * scaled_b),
            col_sum(kda[...] * scaled_a * scaled_a, kdb[...] * scaled_b * scaled_b),
            col_sum(kda[...] * scaled_a * dir_a, kdb[...] * scaled_b * dir_b),
        ),
    )
    v = gathered_product(1, scaled_a, scaled_b, lambda: small_middle(2))

    def finish(new_block, scal):
        ratio = scal[0:1] / norm
        return new_block + ratio * block, scal

    _, scal = slab_values(1, v, small_end(2), finish)
    ratio = scal[0:1] / norm
    norm = scal[0:1]
    diag = scal[1:2] + 2.0 * ratio * scal[2:3] + ratio * ratio * diag
    dir_a, dir_b = scaled_a + ratio * dir_a, scaled_b + ratio * dir_b
    w, last_inner = filtered(2)
    image_a, image_b = scatter(2, w, lambda: small_start(3, rows_of(last_inner)), lambda: small_middle(3), nothing)
    step_len = norm / (diag + small_end(3)[0:1])
    image_a, image_b = image_a + kda[...] * dir_a, image_b + kdb[...] * dir_b
    sol_a, sol_b = sol_a + step_len * dir_a, sol_b + step_len * dir_b
    res_a, res_b = res_a - step_len * image_a, res_b - step_len * image_b
    xout[0:NA] = sol_a[0:NA]
    xout[NA:] = sol_b[0:NB]
    rout[0:NA] = res_a[0:NA]
    rout[NA:] = res_b[0:NB]
    for copy in pending:
        copy.wait_send()


def shards(design, observed, slab_counts, gap_mask, filter_taps, kaula_diag, precond):
    rows = observed.shape[0]
    coefs = design.shape[1]
    dma = pltpu.SemaphoreType.DMA
    args = (
        design, observed, slab_counts, gap_mask.reshape(rows // LANES, LANES), filter_taps.reshape(1, LANES),
        kaula_diag.reshape(coefs // LANES, LANES), precond.reshape(coefs // LANES, LANES),
    )
    vm = pltpu.VMEM
    scratch = [
        vm((NZ, rows, NY * LANES), BF16),
        vm((NY, rows, NZ * LANES), BF16),
        vm((NZ, NY, RA, rows), BF16),
        vm((NY, NZ, RB, rows), BF16),
        vm((rows, LANES), F32),
        vm((RA, LANES), F32), vm((RB, LANES), F32), vm((RA, LANES), F32), vm((RB, LANES), F32),
        vm((4 * LANES, LANES), F32),
        vm((2 * BAND, 4 * BAND), F32), vm((2 * BAND, 4 * BAND), BF16), vm((2 * BAND, 4 * BAND), BF16),
        vm((NZ, NY, RA, 128), F32),
        vm((NZ, RB, 128), F32),
        vm((2, NZ // 2, RB, 128), F32),
        vm((3, 2, 4, NY, RA, 128), I16),
        vm((3, 2, 4, NY, RA, 128), I16),
        vm((3, NY, RA, 128), I16),
        vm((3, NY, RA, 128), I16),
        vm((3, 2, 3, NZ // 2, RB, 128), I16),
        vm((3, 2, 3, NZ // 2, RB, 128), I16),
        vm((3, NZ, RB, 128), I16),
        vm((3, NZ, RB, 128), I16),
        vm((2, NZ, NY, LANES, LANES), BF16),
        vm((2, NY, NZ, LANES, LANES), BF16),
        vm((2, 2, BAND, 128), F32),
        vm((2, BAND, 128), F32),
        vm((2, BAND + 16, 128), I16),
        vm((2, NX, BAND + 16, 128), I16),
        vm((3, 4, BAND + 16, 128), I16),
        vm((4, 2, 8, 128), F32),
        vm((4, NY + NZ, 8, 128), F32),
        vm((2, 2, 8, 128), F32),
        vm((2, NX, 8, 128), F32),
        dma((3, 2, 2)), dma((2, 4, NY)), dma((3,)), dma((NY,)),
        dma((3,)), dma((2, 3)), dma((3,)), dma((NZ,)),
        dma((2, 4)), dma((2, 4, NY)), dma((NY,)), dma((NZ,)), dma((2, 2, NZ)),
        dma((2, 2)), dma((2, 2)), dma((2, 2)), dma((2, NX)), dma((2, NX)), dma((3, 4)), dma((3, 4)),
        dma((4, 2)), dma((4, NY + NZ)),
    ]
    out = jax.ShapeDtypeStruct((OWN, LANES), F32)
    return pl.pallas_call(
        kernel,
        name="cg",
        out_shape=(out, out),
        in_specs=[pl.BlockSpec(memory_space=pltpu.SMEM if i == 2 else vm) for i in range(len(args))],
        out_specs=(pl.BlockSpec(memory_space=vm),) * 2,
        scratch_shapes=scratch,
        compiler_params=pltpu.CompilerParams(
            collective_id=0, has_side_effects=True, vmem_limit_bytes=60 * 1024 * 1024
        ),
    )(*args)


def solution(mesh):
    torus = Mesh(mesh.devices.reshape(NZ, NY, NX, NC), AXES)
    in_specs = (P(TM, COEF), P(TM, None), P(TM), P(TM), P(), P(COEF), P(COEF))
    out_specs = (P((*COEF, *TM), None),) * 2
    return jax.shard_map(shards, mesh=torus, in_specs=in_specs, out_specs=out_specs, check_vma=False)
```

```python
import functools

import jax
import jax.numpy as jnp
from jax import lax
from jax.experimental import pallas as pl
from jax.experimental.pallas import tpu as pltpu
from jax.sharding import Mesh
from jax.sharding import PartitionSpec as P

AXES = ("z", "y", "x", "c")
TM = ("z", "y")
COEF = ("x", "c")
MESH = pl.DeviceIdType.MESH
NZ, NY, NX, NC = 8, 4, 4, 2
NA, NB = 104, 92
RA, RB = 112, 96
OWN = NA + NB
LANES = 128
WIDE = 3 * LANES
I16 = jnp.int16
I32 = jnp.int32
BAND = 128
F32 = jnp.float32
BF16 = jnp.bfloat16
HIGH = lax.Precision.HIGHEST


def dot(a, b, precision=None):
    return jnp.dot(a, b, preferred_element_type=F32, precision=precision)


def dot_t(a, b, precision=None):
    return lax.dot_general(a, b, (((1,), (1,)), ((), ())), preferred_element_type=F32, precision=precision)


def split(v):
    high = v.astype(BF16)
    return high, (v - high.astype(F32)).astype(BF16)


HEADROOM = 0.998


def encoded(v, spare):
    tail = v.shape[-2] - 8
    top = jnp.maximum(jnp.max(jnp.abs(v), axis=-2, keepdims=True), 1e-30)
    power = jnp.floor(jnp.log2(top)) + 1.0
    q = jnp.round(v * (jnp.exp2(15.0 - power) * HEADROOM))
    row = lax.broadcasted_iota(I32, (*v.shape[:-2], 8, v.shape[-1]), v.ndim - 2)
    last = jnp.where(row == spare - tail, power, q[..., tail:, :])
    return jnp.concatenate([q[..., :tail, :], last], -2).astype(I32).astype(I16)


def decoded(q, spare):
    v = q.astype(I32).astype(F32)
    return v * (jnp.exp2(v[..., spare : spare + 1, :] - 15.0) * (1.0 / HEADROOM))


def enc_a(v):
    return encoded(v, NA)


def enc_b(v):
    return encoded(v, NB)


def dec_a(q):
    return decoded(q, NA)


def dec_b(q):
    return decoded(q, NB)


def enc_v(v):
    return encoded(jnp.concatenate([v, jnp.zeros((16, LANES), F32)], 0), BAND + 8)


def dec_v(q):
    return decoded(q, BAND + 8)[..., 0:BAND, :]


def rcopy(src, dst, ssem, rsem, **device):
    return pltpu.make_async_remote_copy(
        src_ref=src, dst_ref=dst, send_sem=ssem, recv_sem=rsem, device_id=device, device_id_type=MESH
    )


def kernel(
    design, obs, counts, gaps, taps, kaula, precond,
    xout, rout,
    aa, ab, ata, atb, wm, kda, kdb, pca, pcb, column, bm, bm_high, bm_low, y_a, y_b, y_c,
    sa, ra, sya, rya, sb, rb, szb, rzb,
    ga, gb, vs, vr, us, ur, hq, scs, scr, scc, scx,
    sem_sa, sem_ra, sem_sya, sem_rya, sem_sb, sem_rb, sem_szb, sem_rzb,
    sem_gs, sem_ga, sem_gay, sem_gb, sem_gby,
    sem_vs, sem_vr, sem_us, sem_ur, sem_uc, sem_hs, sem_hr, sem_cs, sem_cr,
):
    z, y, x, c = (lax.axis_index(name) for name in AXES)
    t = z * NY + y
    zp = [lax.rem(z + k, NZ) for k in range(NZ)]
    zm = [lax.rem(z + NZ - k, NZ) for k in range(NZ)]
    yp = [lax.rem(y + k, NY) for k in range(NY)]
    ym = [lax.rem(y + NY - k, NY) for k in range(NY)]
    xp = [lax.rem(x + k, NX) for k in range(NX)]
    other = 1 - c
    t_up = lax.rem(t + 1, NZ * NY)
    t_down = lax.rem(t + NZ * NY - 1, NZ * NY)
    pending = []

    def send(src, dst, ssem, rsem, **device):
        rcopy(src, dst, ssem, rsem, **device).start()

    def sent(ref, sem):
        pending.append(rcopy(ref, ref, sem, sem, c=other))

    def arrived(dst, ssem, rsem, **device):
        rcopy(dst, dst, ssem, rsem, **device).wait_recv()

    barrier = pltpu.get_barrier_semaphore()
    peers = [dict(z=zp[k]) for k in range(1, NZ)] + [dict(y=yp[k]) for k in range(1, NY)]
    peers += [dict(x=xp[k]) for k in range(1, NX)] + [dict(c=other)]
    for step in (t_up, t_down):
        for core in range(NC):
            peers.append(dict(z=lax.div(step, NY), y=lax.rem(step, NY), c=jnp.int32(core)))
    for peer in peers:
        pl.semaphore_signal(barrier, inc=1, device_id=peer, device_id_type=MESH)

    row = lax.broadcasted_iota(I32, (BAND, BAND), 0)
    col = lax.broadcasted_iota(I32, (BAND, BAND), 1)
    for b in range(2):
        on = (gaps[b : b + 1, :] == 1) & (col[0:1] + b * BAND < counts[0])
        wm[b * BAND : (b + 1) * BAND] = jnp.broadcast_to(jnp.where(on, 1.0, 0.0), (BAND, BAND)).T

    for b in range(2):
        hq[0, 1 + b] = enc_v(wm[b * BAND : (b + 1) * BAND] * obs[b * BAND : (b + 1) * BAND])
    def picked(p):
        first = jnp.minimum(lax.div(p * OWN, LANES), design.shape[1] // LANES - 3)
        window = design[:, pl.ds(pl.multiple_of(first * LANES, LANES), WIDE)]
        place = lax.broadcasted_iota(I32, (2 * LANES, WIDE), 0)
        wanted = jnp.where(place < LANES, place, place - LANES + NA)
        real = ((place < NA) | (place >= LANES)) & (place < LANES + NB)
        at = lax.broadcasted_iota(I32, (2 * LANES, WIDE), 1) - (p * OWN - first * LANES)
        return window, jnp.where((at == wanted) & real, 1.0, 0.0).astype(BF16)

    def put_rows(p, carry):
        window, pick = picked(p)
        rows = dot_t(pick, window).astype(BF16)
        zz, yy = lax.div(p, NY), lax.rem(p, NY)
        ata[zz, yy] = rows[0:RA]
        atb[yy, zz] = rows[LANES : LANES + RB]
        return carry

    def put_columns(p, carry):
        window, pick = picked(p)
        columns = dot_t(window, pick).astype(BF16)
        zz, yy = lax.div(p, NY), lax.rem(p, NY)
        aa[zz, :, pl.ds(pl.multiple_of(yy * LANES, LANES), LANES)] = columns[:, 0:LANES]
        ab[yy, :, pl.ds(pl.multiple_of(zz * LANES, LANES), LANES)] = columns[:, LANES:]
        for it in range(2):
            ga[it, zz, yy, RA:] = jnp.zeros((LANES - RA, LANES), BF16)
            gb[it, yy, zz, RB:] = jnp.zeros((LANES - RB, LANES), BF16)
        return carry

    def at_a(target):
        return ata[target].reshape(NY * RA, 2 * BAND)

    def at_b(target):
        return atb[target].reshape(NZ * RB, 2 * BAND)

    def put_four(i, carry):
        for k in range(4):
            put_rows(4 * i + k, carry)
        return carry

    early_fours = 4
    lax.fori_loop(0, early_fours, put_four, 0)
    pl.semaphore_wait(barrier, len(peers))
    for place, goal, step in ((2, 0, t_up), (1, 3, t_down)):
        send(
            hq.at[0, place], hq.at[0, goal], sem_hs.at[0, goal], sem_hr.at[0, goal],
            z=lax.div(step, NY), y=lax.rem(step, NY),
        )
        sent(hq.at[0, place], sem_hs.at[0, goal])

    keep_first = jnp.where(t == 0, 0.0, 1.0).astype(F32)
    keep_last = jnp.where(t == NZ * NY - 1, 0.0, 1.0).astype(F32)
    rolled = pltpu.roll(jnp.broadcast_to(taps[...], (BAND, BAND)), 0, 1, stride=1, stride_axis=0)
    lot = jnp.where(col >= row, rolled, 0.0)
    upt = jnp.where(col < row, rolled, 0.0)
    ll = dot_t(lot, lot, HIGH)
    uu = dot_t(upt, upt, HIGH)
    lu = dot_t(lot, upt, HIGH)
    ul = dot_t(upt, lot, HIGH)
    zero = jnp.zeros((BAND, BAND), F32)
    bm[0:BAND, 0:BAND] = keep_first * lu
    bm[0:BAND, BAND : 2 * BAND] = ll + uu
    bm[0:BAND, 2 * BAND : 3 * BAND] = ul
    bm[0:BAND, 3 * BAND :] = zero
    bm[BAND:, 0:BAND] = zero
    bm[BAND:, BAND : 2 * BAND] = lu
    bm[BAND:, 2 * BAND : 3 * BAND] = ll + keep_last * uu
    bm[BAND:, 3 * BAND :] = keep_last * ul
    bm_high[...], bm_low[...] = split(bm[...])

    line = lax.div(t * OWN, LANES)
    shift = t * OWN - line * LANES
    for diag, part_a, part_b in ((kaula, kda, kdb), (precond, pca, pcb)):
        for k in range(3):
            values = diag[pl.ds(jnp.minimum(line + k, diag.shape[0] - 1), 1), :]
            column[k * LANES : (k + 1) * LANES] = jnp.broadcast_to(values, (LANES, LANES)).T
        row_a = lax.broadcasted_iota(I32, (RA, LANES), 0)
        row_b = lax.broadcasted_iota(I32, (RB, LANES), 0)
        part_a[...] = jnp.where(row_a < NA, column[pl.ds(shift, RA), :], 0.0)
        part_b[...] = jnp.where(row_b < NB, column[pl.ds(shift + NA, RB), :], 0.0)

    lax.fori_loop(early_fours, NZ * NY // 4, put_four, 0)

    def filtered(st):
        ext = dec_v(hq[st])
        high, low = split(ext.reshape(4 * BAND, BAND))
        series = dot(bm_high[...], high) + (dot(bm_high[...], low) + dot(bm_low[...], high))
        w = (wm[...] * series).astype(BF16)
        inner = ext[1] * w[0:BAND].astype(F32) + ext[2] * w[BAND:].astype(F32)
        return w, jnp.sum(inner, 0, keepdims=True)

    def small_start(i, block):
        scs[i, 0] = block
        for k in range(1, NY):
            send(scs.at[i, 0], scr.at[i, k], sem_cs.at[i, 0], sem_cr.at[i, k], y=yp[k])

    def small_middle(i):
        sent(scr.at[i, pl.ds(0, NY - 1)], sem_cs.at[i, 0])
        total = scs[i, 0]
        for k in range(1, NY):
            arrived(scr.at[i, k], sem_cs.at[i, 0], sem_cr.at[i, k], y=yp[k])
            total = total + scr[i, k]
        scs[i, 1] = total
        for k in range(1, NZ):
            send(scs.at[i, 1], scr.at[i, NY + k], sem_cs.at[i, 1], sem_cr.at[i, NY + k], z=zp[k])

    def small_end(i):
        sent(scr.at[i, pl.ds(0, NZ - 1)], sem_cs.at[i, 1])
        total = scs[i, 1]
        for k in range(1, NZ):
            arrived(scr.at[i, NY + k], sem_cs.at[i, 1], sem_cr.at[i, NY + k], z=zp[k])
            total = total + scr[i, NY + k]
        return total

    half = NZ // 2 * RB

    def long_way(j):
        return 0 if j in (0, 3) else 1

    def along_z(way, links):
        return zp[links] if way == 0 else zm[links]

    def scatter(st, w, early, late, fill):
        ways_y = ((0, yp[1]), (1, ym[1]))

        def send_b(way, kind, peer):
            send(sb.at[st, way, kind], rb.at[st, way, kind], sem_sb.at[st], sem_rb.at[way, kind], y=peer)

        def got_b(way, kind):
            arrived(rb.at[st, way, kind], sem_sb.at[st], sem_rb.at[way, kind], y=yp[1])

        def send_a(way, s, j):
            send(
                sa.at[st, way, s, j], ra.at[st, way, s, j], sem_sa.at[st, way, abs(long_way(j) - way)],
                sem_ra.at[way, s, j], z=along_z(way, 2 if s == 0 else 1),
            )

        def got_a(way, s, j):
            arrived(ra.at[st, way, s, j], sem_sa.at[st, way, 0], sem_ra.at[way, s, j], z=zp[1])

        part = dot(at_b(yp[2]), w).reshape(2, NZ // 2, RB, 128)
        for way, peer in ways_y:
            sb[st, way, 0] = enc_b(part[way])
            send_b(way, 0, peer)
        far = enc_a(dot(at_a(zp[4]), w).reshape(NY, RA, 128))
        for j in range(NY):
            sa[st, long_way(j), 0, j] = far[j]
            send_a(long_way(j), 0, j)
        for way in range(2):
            sa[st, way, 1] = enc_a(dot(at_a(along_z(way, 3)), w).reshape(NY, RA, 128))
            for j in range(NY):
                send_a(way, 1, j)
        for way, peer in ways_y:
            part = dot(at_b(peer), w).reshape(2, NZ // 2, RB, 128)
            sb[st, way, 1] = enc_b(part[1 - way])
            send_b(way, 1, peer)
            y_c[way] = part[way]

        def product(i, carry):
            target = lax.rem(z + NZ - 2 + i, NZ)
            y_a[target] = dot(at_a(target), w).reshape(NY, RA, 128)
            return carry

        lax.fori_loop(0, 5, product, 0)
        y_b[...] = dot(at_b(y), w).reshape(NZ, RB, 128)
        early()
        for i in range(2):
            fill(i)

        def pass_on(s, j):
            codes = []
            for way in range(2):
                got_a(way, s - 1, j)
                if s == 2 and way == long_way(j):
                    got_a(way, 0, j)
            for way in range(2):
                total = dec_a(ra[st, way, s - 1, j]) + y_a[along_z(way, 4 - s), j]
                if s == 2 and way == long_way(j):
                    total = total + dec_a(ra[st, way, 0, j])
                codes.append(enc_a(total))
            for way in range(2):
                sa[st, way, s, j] = codes[way]
            for way in range(2):
                send_a(way, s, j)

        for j in range(NY):
            pass_on(2, j)
        for way, peer in ways_y:
            got_b(way, 0)
            sb[st, way, 2] = enc_b(y_c[way] + dec_b(rb[st, way, 0]))
            send_b(way, 2, peer)
        fill(2)
        for j in range(NY):
            pass_on(3, j)
        late()
        for i in range(3, 6):
            fill(i)
        for way in range(2):
            for kind in (1, 2):
                got_b(way, kind)
        low = y_b[0 : NZ // 2] + dec_b(rb[st, 0, 2]) + dec_b(rb[st, 1, 1])
        y_b[0 : NZ // 2] = low
        szb[st, 0 : NZ // 2] = enc_b(low)
        high = y_b[NZ // 2 :] + dec_b(rb[st, 0, 1]) + dec_b(rb[st, 1, 2])
        y_b[NZ // 2 :] = high
        szb[st, NZ // 2 :] = enc_b(high)
        for k in (4, 3, 5, 2, 6, 1, 7):
            send(szb.at[st, zp[k]], rzb.at[st, k], sem_szb.at[st], sem_rzb.at[k], z=zp[k])
        for j in range(NY):
            for way in range(2):
                got_a(way, 3, j)
            total = dec_a(ra[st, 0, 3, j]) + dec_a(ra[st, 1, 3, j]) + y_a[z, j]
            y_a[z, j] = total
            sya[st, j] = enc_a(total)
        for k in (2, 1, 3):
            send(sya.at[st, yp[k]], rya.at[st, k], sem_sya.at[st], sem_rya.at[k], y=yp[k])
        for i in range(6, 11):
            fill(i)
        sum_b = y_b[z]
        for k in range(1, NZ):
            arrived(rzb.at[st, k], sem_szb.at[st], sem_rzb.at[k], z=zp[k])
            sum_b = sum_b + dec_b(rzb[st, k])
        sum_a = y_a[z, y]
        for k in range(1, NY):
            arrived(rya.at[st, k], sem_sya.at[st], sem_rya.at[k], y=yp[k])
            sum_a = sum_a + dec_a(rya[st, k])
        for way in range(2):
            sent(sa.at[st, way, :, pl.ds(0, 2)], sem_sa.at[st, way, 0])
            sent(sa.at[st, way, pl.ds(0, 3), pl.ds(0, 2)], sem_sa.at[st, way, 1])
        sent(sb.at[st], sem_sb.at[st])
        sent(szb.at[st, pl.ds(0, NZ - 1)], sem_szb.at[st])
        sent(sya.at[st, pl.ds(0, NY - 1)], sem_sya.at[st])
        return sum_a, sum_b

    first_half, second_half = (0, 1, 7, 2), (6, 3, 5, 4)

    def gathered_product(it, rows_a, rows_b, middle):
        ga[it, z, y, 0:RA] = rows_a.astype(BF16)
        gb[it, y, z, 0:RB] = rows_b.astype(BF16)

        def part_a(it, zz, yy):
            return ga.at[it, zz, yy, pl.ds(0, RA)]

        def part_b(it, yy, zz):
            return gb.at[it, yy, zz, pl.ds(0, RB)]

        def put_a(way, s, k):
            block = part_a(it, along_z(1 - way, s - 1 if s else 2), ym[k])
            send(block, block, sem_gs.at[it, 0], sem_ga.at[way, s, k], z=along_z(way, 1 if s else 2))

        def got_a(way, s, k):
            block = part_a(it, along_z(1 - way, s if s else 4), ym[k])
            arrived(block, sem_gs.at[it, 0], sem_ga.at[way, s, k], z=zp[1])

        def put_b(way, s, k):
            block = part_b(it, ym[s] if way == 0 else yp[s], zm[k])
            send(block, block, sem_gs.at[it, 1], sem_gby.at[way, s, k], y=yp[1] if way == 0 else ym[1])

        def got_b(way, s, k):
            block = part_b(it, ym[s + 1] if way == 0 else yp[s + 1], zm[k])
            arrived(block, sem_gs.at[it, 1], sem_gby.at[way, s, k], y=yp[1])

        def from_z(k):
            arrived(part_b(it, y, zm[k]), sem_gs.at[it, 3], sem_gb.at[k], z=zp[k])
            if k == 5:
                send(part_b(it, y, zm[5]), part_b(it, y, zm[5]), sem_gs.at[it, 3], sem_gb.at[4], z=zm[1])
            put_b(0, 0, k)
            put_b(1, 0, k)

        own_a, own_b = part_a(it, z, y), part_b(it, y, z)
        for k in (2, 1, 3):
            send(own_a, own_a, sem_gs.at[it, 2], sem_gay.at[k], y=yp[k])
        put_a(0, 1, 0)
        put_a(1, 1, 0)
        for k in (5, 3, 2, 6, 1, 7):
            send(own_b, own_b, sem_gs.at[it, 3], sem_gb.at[k], z=zp[k])
        put_b(0, 0, 0)
        put_b(1, 0, 0)
        def pass_a(s, blocks):
            for k in blocks:
                for way in range(2):
                    got_a(way, s, k)
                    if s == 2 and way == long_way(k):
                        put_a(way, 0, k)
                    if s < 3:
                        put_a(way, s + 1, k)

        def pass_b(blocks):
            for k in blocks:
                way = 0 if k in first_half else 1
                got_b(way, 0, k)
                put_b(way, 1, k)

        def times_a(v, zz):
            return v + dot(aa[zz], ga[it, zz].reshape(NY * LANES, LANES))

        def times_b(v, yy):
            return v + dot(ab[yy], gb[it, yy].reshape(NZ * LANES, LANES))

        for k in (1, 3, 2):
            arrived(part_a(it, z, ym[k]), sem_gs.at[it, 2], sem_gay.at[k], y=yp[k])
            put_a(0, 1, k)
            put_a(1, 1, k)
        pass_a(1, (0,))
        pass_b((0,))
        for k in (1, 7, 2, 6):
            from_z(k)
        middle()
        for k in (5, 3):
            from_z(k)
        v = dot(aa[z], ga[it, z].reshape(NY * LANES, LANES))
        pass_a(1, (1, 3, 2))
        pass_a(2, (0,))
        pass_b((1, 7, 2, 6))
        v = times_a(times_a(v, zm[1]), zp[1])
        pass_b((5, 3))
        from_z(4)
        pass_a(2, (1, 3, 2))
        pass_a(3, (0,))
        v = times_b(times_a(times_a(v, zm[2]), zp[2]), y)
        pass_b((4,))
        for k in second_half:
            got_b(0, 0, k)
        for k in first_half:
            got_b(1, 0, k)
        v = times_b(times_b(v, yp[1]), ym[1])
        pass_a(3, (1, 3, 2))
        v = times_a(times_a(v, zm[3]), zp[3])
        for k in first_half:
            got_b(0, 1, k)
        for k in second_half:
            got_b(1, 1, k)
        v = times_b(v, yp[2])
        for k in range(NY):
            got_a(long_way(k), 0, k)
        sent(ga.at[it, pl.ds(0, NZ - 1), :, pl.ds(0, RA)], sem_gs.at[it, 0])
        sent(gb.at[it, pl.ds(0, NY - 1), :, pl.ds(0, RB)], sem_gs.at[it, 1])
        sent(ga.at[it, 0, pl.ds(0, NY - 1), pl.ds(0, RA)], sem_gs.at[it, 2])
        sent(gb.at[it, 0, pl.ds(0, NZ - 1), pl.ds(0, RB)], sem_gs.at[it, 3])
        return v + dot(aa[zm[4]], ga[it, zm[4]].reshape(NY * LANES, LANES))

    def slab_values(it, v, scal, finish):
        vs[it] = v.reshape(2, BAND, 128)
        scc[it, 0] = scal
        send(vs.at[it, other], vr.at[it], sem_vs.at[it, 0], sem_vr.at[it, 0], c=other)
        send(scc.at[it, 0], scc.at[it, 1], sem_vs.at[it, 1], sem_vr.at[it, 1], c=other)
        arrived(vr.at[it], sem_vs.at[it, 0], sem_vr.at[it, 0], c=other)
        chip = vs[it, c] + vr[it]
        us[it] = enc_v(chip)
        for k in (2, 1, 3):
            send(us.at[it], ur.at[it, k], sem_us.at[it, 0], sem_ur.at[it, k], x=xp[k])
        arrived(scc.at[it, 1], sem_vs.at[it, 1], sem_vr.at[it, 1], c=other)
        scal = scc[it, 0] + scc[it, 1]
        scx[it, 0] = scal
        for k in (2, 1, 3):
            send(scx.at[it, 0], scx.at[it, k], sem_us.at[it, 1], sem_uc.at[it, k], x=xp[k])
        for k in range(1, NX):
            arrived(ur.at[it, k], sem_us.at[it, 0], sem_ur.at[it, k], x=xp[k])
            chip = chip + dec_v(ur[it, k])
            arrived(scx.at[it, k], sem_us.at[it, 1], sem_uc.at[it, k], x=xp[k])
            scal = scal + scx[it, k]
        mask = wm[pl.ds(pl.multiple_of(c * BAND, BAND), BAND), :]
        block, scal = finish(mask * chip, scal)
        hq[it + 1, 1 + c] = enc_v(block)
        slot = 3 - 3 * c
        step = jnp.where(c == 0, t_down, t_up)
        mine = hq.at[it + 1, 1 + c]
        for core in range(NC):
            send(
                mine, hq.at[it + 1, slot], sem_hs.at[it + 1, 1 + core], sem_hr.at[it + 1, slot],
                z=lax.div(step, NY), y=lax.rem(step, NY), c=jnp.int32(core),
            )
        send(mine, mine, sem_hs.at[it + 1, 0], sem_hr.at[it + 1, 1 + c], c=other)
        for k in range(3):
            sent(mine, sem_hs.at[it + 1, k])
        sent(vs.at[it, 0], sem_vs.at[it, 0])
        sent(scc.at[it, 0], sem_vs.at[it, 1])
        sent(ur.at[it, pl.ds(0, NX - 1)], sem_us.at[it, 0])
        sent(scx.at[it, pl.ds(0, NX - 1)], sem_us.at[it, 1])
        for place in (2 - c, 0, 3):
            arrived(hq.at[it + 1, place], sem_hs.at[it + 1, 0], sem_hr.at[it + 1, place], c=other)
        return block, scal

    arrived(hq.at[0, 0], sem_hs.at[0, 0], sem_hr.at[0, 0], c=other)
    arrived(hq.at[0, 3], sem_hs.at[0, 0], sem_hr.at[0, 3], c=other)

    def nothing(*_):
        return None

    def some_columns(i):
        lax.fori_loop(3 * i, min(3 * i + 3, NZ * NY), put_columns, 0)

    w, _ = filtered(0)
    res_a, res_b = scatter(0, w, nothing, nothing, some_columns)

    def col_sum(a, b):
        return jnp.sum(a, 0, keepdims=True) + jnp.sum(b, 0, keepdims=True)

    def rows_of(*rows):
        spare = jnp.zeros((8 - len(rows), 128), F32)
        return jnp.concatenate([*rows, spare], 0)

    dir_a, dir_b = pca[...] * res_a, pcb[...] * res_b
    small_start(0, rows_of(col_sum(res_a * dir_a, res_b * dir_b), col_sum(kda[...] * dir_a * dir_a, kdb[...] * dir_b * dir_b)))
    v = gathered_product(0, dir_a, dir_b, lambda: small_middle(0))
    block, scal = slab_values(0, v, small_end(0), lambda block, scal: (block, scal))
    norm, diag = scal[0:1], scal[1:2]

    w, inner = filtered(1)
    image_a, image_b = scatter(1, w, lambda: small_start(1, rows_of(inner)), lambda: small_middle(1), nothing)
    step_len = norm / (diag + small_end(1)[0:1])
    image_a, image_b = image_a + kda[...] * dir_a, image_b + kdb[...] * dir_b
    sol_a, sol_b = step_len * dir_a, step_len * dir_b
    res_a, res_b = res_a - step_len * image_a, res_b - step_len * image_b
    scaled_a, scaled_b = pca[...] * res_a, pcb[...] * res_b
    small_start(
        2,
        rows_of(
            col_sum(res_a * scaled_a, res_b * scaled_b),
            col_sum(kda[...] * scaled_a * scaled_a, kdb[...] * scaled_b * scaled_b),
            col_sum(kda[...] * scaled_a * dir_a, kdb[...] * scaled_b * dir_b),
        ),
    )
    v = gathered_product(1, scaled_a, scaled_b, lambda: small_middle(2))

    def finish(new_block, scal):
        ratio = scal[0:1] / norm
        return new_block + ratio * block, scal

    _, scal = slab_values(1, v, small_end(2), finish)
    ratio = scal[0:1] / norm
    norm = scal[0:1]
    diag = scal[1:2] + 2.0 * ratio * scal[2:3] + ratio * ratio * diag
    dir_a, dir_b = scaled_a + ratio * dir_a, scaled_b + ratio * dir_b
    w, last_inner = filtered(2)
    image_a, image_b = scatter(2, w, lambda: small_start(3, rows_of(last_inner)), lambda: small_middle(3), nothing)
    step_len = norm / (diag + small_end(3)[0:1])
    image_a, image_b = image_a + kda[...] * dir_a, image_b + kdb[...] * dir_b
    sol_a, sol_b = sol_a + step_len * dir_a, sol_b + step_len * dir_b
    res_a, res_b = res_a - step_len * image_a, res_b - step_len * image_b
    xout[0:NA] = sol_a[0:NA]
    xout[NA:] = sol_b[0:NB]
    rout[0:NA] = res_a[0:NA]
    rout[NA:] = res_b[0:NB]
    for copy in pending:
        copy.wait_send()


def shards(design, observed, slab_counts, gap_mask, filter_taps, kaula_diag, precond):
    rows = observed.shape[0]
    coefs = design.shape[1]
    dma = pltpu.SemaphoreType.DMA
    args = (
        design, observed, slab_counts, gap_mask.reshape(rows // LANES, LANES), filter_taps.reshape(1, LANES),
        kaula_diag.reshape(coefs // LANES, LANES), precond.reshape(coefs // LANES, LANES),
    )
    vm = pltpu.VMEM
    scratch = [
        vm((NZ, rows, NY * LANES), BF16),
        vm((NY, rows, NZ * LANES), BF16),
        vm((NZ, NY, RA, rows), BF16),
        vm((NY, NZ, RB, rows), BF16),
        vm((rows, LANES), F32),
        vm((RA, LANES), F32), vm((RB, LANES), F32), vm((RA, LANES), F32), vm((RB, LANES), F32),
        vm((4 * LANES, LANES), F32),
        vm((2 * BAND, 4 * BAND), F32), vm((2 * BAND, 4 * BAND), BF16), vm((2 * BAND, 4 * BAND), BF16),
        vm((NZ, NY, RA, 128), F32),
        vm((NZ, RB, 128), F32),
        vm((2, NZ // 2, RB, 128), F32),
        vm((3, 2, 4, NY, RA, 128), I16),
        vm((3, 2, 4, NY, RA, 128), I16),
        vm((3, NY, RA, 128), I16),
        vm((3, NY, RA, 128), I16),
        vm((3, 2, 3, NZ // 2, RB, 128), I16),
        vm((3, 2, 3, NZ // 2, RB, 128), I16),
        vm((3, NZ, RB, 128), I16),
        vm((3, NZ, RB, 128), I16),
        vm((2, NZ, NY, LANES, LANES), BF16),
        vm((2, NY, NZ, LANES, LANES), BF16),
        vm((2, 2, BAND, 128), F32),
        vm((2, BAND, 128), F32),
        vm((2, BAND + 16, 128), I16),
        vm((2, NX, BAND + 16, 128), I16),
        vm((3, 4, BAND + 16, 128), I16),
        vm((4, 2, 8, 128), F32),
        vm((4, NY + NZ, 8, 128), F32),
        vm((2, 2, 8, 128), F32),
        vm((2, NX, 8, 128), F32),
        dma((3, 2, 2)), dma((2, 4, NY)), dma((3,)), dma((NY,)),
        dma((3,)), dma((2, 3)), dma((3,)), dma((NZ,)),
        dma((2, 4)), dma((2, 4, NY)), dma((NY,)), dma((NZ,)), dma((2, 2, NZ)),
        dma((2, 2)), dma((2, 2)), dma((2, 2)), dma((2, NX)), dma((2, NX)), dma((3, 4)), dma((3, 4)),
        dma((4, 2)), dma((4, NY + NZ)),
    ]
    out = jax.ShapeDtypeStruct((OWN, LANES), F32)
    return pl.pallas_call(
        kernel,
        name="cg",
        out_shape=(out, out),
        in_specs=[pl.BlockSpec(memory_space=pltpu.SMEM if i == 2 else vm) for i in range(len(args))],
        out_specs=(pl.BlockSpec(memory_space=vm),) * 2,
        scratch_shapes=scratch,
        compiler_params=pltpu.CompilerParams(
            collective_id=0, has_side_effects=True, vmem_limit_bytes=60 * 1024 * 1024
        ),
    )(*args)


def solution(mesh):
    torus = Mesh(mesh.devices.reshape(NZ, NY, NX, NC), AXES)
    in_specs = (P(TM, COEF), P(TM, None), P(TM), P(TM), P(), P(COEF), P(COEF))
    out_specs = (P((*COEF, *TM), None),) * 2
    return jax.shard_map(shards, mesh=torus, in_specs=in_specs, out_specs=out_specs, check_vma=False)
```

```python
import functools

import jax
import jax.numpy as jnp
from jax import lax
from jax.experimental import pallas as pl
from jax.experimental.pallas import tpu as pltpu
from jax.sharding import Mesh
from jax.sharding import PartitionSpec as P

AXES = ("z", "y", "x", "c")
TM = ("z", "y")
COEF = ("x", "c")
MESH = pl.DeviceIdType.MESH
NZ, NY, NX, NC = 8, 4, 4, 2
NA, NB = 104, 92
RA, RB = 112, 96
OWN = NA + NB
LANES = 128
WIDE = 3 * LANES
I16 = jnp.int16
I32 = jnp.int32
BAND = 128
F32 = jnp.float32
BF16 = jnp.bfloat16
HIGH = lax.Precision.HIGHEST


def dot(a, b, precision=None):
    return jnp.dot(a, b, preferred_element_type=F32, precision=precision)


def dot_t(a, b, precision=None):
    return lax.dot_general(a, b, (((1,), (1,)), ((), ())), preferred_element_type=F32, precision=precision)


def split(v):
    high = v.astype(BF16)
    return high, (v - high.astype(F32)).astype(BF16)


HEADROOM = 0.998


def encoded(v, spare):
    tail = v.shape[-2] - 8
    top = jnp.maximum(jnp.max(jnp.abs(v), axis=-2, keepdims=True), 1e-30)
    power = jnp.floor(jnp.log2(top)) + 1.0
    q = jnp.round(v * (jnp.exp2(15.0 - power) * HEADROOM))
    row = lax.broadcasted_iota(I32, (*v.shape[:-2], 8, v.shape[-1]), v.ndim - 2)
    last = jnp.where(row == spare - tail, power, q[..., tail:, :])
    return jnp.concatenate([q[..., :tail, :], last], -2).astype(I32).astype(I16)


def decoded(q, spare):
    v = q.astype(I32).astype(F32)
    return v * (jnp.exp2(v[..., spare : spare + 1, :] - 15.0) * (1.0 / HEADROOM))


def enc_a(v):
    return encoded(v, NA)


def enc_b(v):
    return encoded(v, NB)


def dec_a(q):
    return decoded(q, NA)


def dec_b(q):
    return decoded(q, NB)


def enc_v(v):
    return encoded(jnp.concatenate([v, jnp.zeros((16, LANES), F32)], 0), BAND + 8)


def dec_v(q):
    return decoded(q, BAND + 8)[..., 0:BAND, :]


def rcopy(src, dst, ssem, rsem, **device):
    return pltpu.make_async_remote_copy(
        src_ref=src, dst_ref=dst, send_sem=ssem, recv_sem=rsem, device_id=device, device_id_type=MESH
    )


def kernel(
    design, obs, counts, gaps, taps, kaula, precond,
    xout, rout,
    aa, ab, ata, atb, wm, kda, kdb, pca, pcb, column, bm, bm_high, bm_low, y_a, y_b, y_c,
    sa, ra, sya, rya, sb, rb, szb, rzb,
    ga, gb, vs, vr, us, ur, hq, scs, scr, scc, scx,
    sem_sa, sem_ra, sem_sya, sem_rya, sem_sb, sem_rb, sem_szb, sem_rzb,
    sem_gs, sem_ga, sem_gay, sem_gb, sem_gby,
    sem_vs, sem_vr, sem_us, sem_ur, sem_uc, sem_hs, sem_hr, sem_cs, sem_cr,
):
    z, y, x, c = (lax.axis_index(name) for name in AXES)
    t = z * NY + y
    zp = [lax.rem(z + k, NZ) for k in range(NZ)]
    zm = [lax.rem(z + NZ - k, NZ) for k in range(NZ)]
    yp = [lax.rem(y + k, NY) for k in range(NY)]
    ym = [lax.rem(y + NY - k, NY) for k in range(NY)]
    xp = [lax.rem(x + k, NX) for k in range(NX)]
    other = 1 - c
    t_up = lax.rem(t + 1, NZ * NY)
    t_down = lax.rem(t + NZ * NY - 1, NZ * NY)
    pending = []

    def send(src, dst, ssem, rsem, **device):
        rcopy(src, dst, ssem, rsem, **device).start()

    def sent(ref, sem):
        pending.append(rcopy(ref, ref, sem, sem, c=other))

    def arrived(dst, ssem, rsem, **device):
        rcopy(dst, dst, ssem, rsem, **device).wait_recv()

    barrier = pltpu.get_barrier_semaphore()
    peers = [dict(z=zp[k]) for k in range(1, NZ)] + [dict(y=yp[k]) for k in range(1, NY)]
    peers += [dict(x=xp[k]) for k in range(1, NX)] + [dict(c=other)]
    for step in (t_up, t_down):
        for core in range(NC):
            peers.append(dict(z=lax.div(step, NY), y=lax.rem(step, NY), c=jnp.int32(core)))
    for peer in peers:
        pl.semaphore_signal(barrier, inc=1, device_id=peer, device_id_type=MESH)

    row = lax.broadcasted_iota(I32, (BAND, BAND), 0)
    col = lax.broadcasted_iota(I32, (BAND, BAND), 1)
    for b in range(2):
        on = (gaps[b : b + 1, :] == 1) & (col[0:1] + b * BAND < counts[0])
        wm[b * BAND : (b + 1) * BAND] = jnp.broadcast_to(jnp.where(on, 1.0, 0.0), (BAND, BAND)).T

    for b in range(2):
        hq[0, 1 + b] = enc_v(wm[b * BAND : (b + 1) * BAND] * obs[b * BAND : (b + 1) * BAND])
    def picked(p):
        first = jnp.minimum(lax.div(p * OWN, LANES), design.shape[1] // LANES - 3)
        window = design[:, pl.ds(pl.multiple_of(first * LANES, LANES), WIDE)]
        place = lax.broadcasted_iota(I32, (2 * LANES, WIDE), 0)
        wanted = jnp.where(place < LANES, place, place - LANES + NA)
        real = ((place < NA) | (place >= LANES)) & (place < LANES + NB)
        at = lax.broadcasted_iota(I32, (2 * LANES, WIDE), 1) - (p * OWN - first * LANES)
        return window, jnp.where((at == wanted) & real, 1.0, 0.0).astype(BF16)

    def put_rows(p, carry):
        window, pick = picked(p)
        rows = dot_t(pick, window).astype(BF16)
        zz, yy = lax.div(p, NY), lax.rem(p, NY)
        ata[zz, yy] = rows[0:RA]
        atb[yy, zz] = rows[LANES : LANES + RB]
        return carry

    def put_columns(p, carry):
        window, pick = picked(p)
        columns = dot_t(window, pick).astype(BF16)
        zz, yy = lax.div(p, NY), lax.rem(p, NY)
        aa[zz, :, pl.ds(pl.multiple_of(yy * LANES, LANES), LANES)] = columns[:, 0:LANES]
        ab[yy, :, pl.ds(pl.multiple_of(zz * LANES, LANES), LANES)] = columns[:, LANES:]
        for it in range(2):
            ga[it, zz, yy, RA:] = jnp.zeros((LANES - RA, LANES), BF16)
            gb[it, yy, zz, RB:] = jnp.zeros((LANES - RB, LANES), BF16)
        return carry

    def at_a(target):
        return ata[target].reshape(NY * RA, 2 * BAND)

    def at_b(target):
        return atb[target].reshape(NZ * RB, 2 * BAND)

    def put_four(i, carry):
        for k in range(4):
            put_rows(4 * i + k, carry)
        return carry

    early_fours = 4
    lax.fori_loop(0, early_fours, put_four, 0)
    pl.semaphore_wait(barrier, len(peers))
    for place, goal, step in ((2, 0, t_up), (1, 3, t_down)):
        send(
            hq.at[0, place], hq.at[0, goal], sem_hs.at[0, goal], sem_hr.at[0, goal],
            z=lax.div(step, NY), y=lax.rem(step, NY),
        )
        sent(hq.at[0, place], sem_hs.at[0, goal])

    keep_first = jnp.where(t == 0, 0.0, 1.0).astype(F32)
    keep_last = jnp.where(t == NZ * NY - 1, 0.0, 1.0).astype(F32)
    rolled = pltpu.roll(jnp.broadcast_to(taps[...], (BAND, BAND)), 0, 1, stride=1, stride_axis=0)
    lot = jnp.where(col >= row, rolled, 0.0)
    upt = jnp.where(col < row, rolled, 0.0)
    ll = dot_t(lot, lot, HIGH)
    uu = dot_t(upt, upt, HIGH)
    lu = dot_t(lot, upt, HIGH)
    ul = dot_t(upt, lot, HIGH)
    zero = jnp.zeros((BAND, BAND), F32)
    bm[0:BAND, 0:BAND] = keep_first * lu
    bm[0:BAND, BAND : 2 * BAND] = ll + uu
    bm[0:BAND, 2 * BAND : 3 * BAND] = ul
    bm[0:BAND, 3 * BAND :] = zero
    bm[BAND:, 0:BAND] = zero
    bm[BAND:, BAND : 2 * BAND] = lu
    bm[BAND:, 2 * BAND : 3 * BAND] = ll + keep_last * uu
    bm[BAND:, 3 * BAND :] = keep_last * ul
    bm_high[...], bm_low[...] = split(bm[...])

    line = lax.div(t * OWN, LANES)
    shift = t * OWN - line * LANES
    for diag, part_a, part_b in ((kaula, kda, kdb), (precond, pca, pcb)):
        for k in range(3):
            values = diag[pl.ds(jnp.minimum(line + k, diag.shape[0] - 1), 1), :]
            column[k * LANES : (k + 1) * LANES] = jnp.broadcast_to(values, (LANES, LANES)).T
        row_a = lax.broadcasted_iota(I32, (RA, LANES), 0)
        row_b = lax.broadcasted_iota(I32, (RB, LANES), 0)
        part_a[...] = jnp.where(row_a < NA, column[pl.ds(shift, RA), :], 0.0)
        part_b[...] = jnp.where(row_b < NB, column[pl.ds(shift + NA, RB), :], 0.0)

    lax.fori_loop(early_fours, NZ * NY // 4, put_four, 0)

    def filtered(st):
        ext = dec_v(hq[st])
        high, low = split(ext.reshape(4 * BAND, BAND))
        series = dot(bm_high[...], high) + (dot(bm_high[...], low) + dot(bm_low[...], high))
        w = (wm[...] * series).astype(BF16)
        inner = ext[1] * w[0:BAND].astype(F32) + ext[2] * w[BAND:].astype(F32)
        return w, jnp.sum(inner, 0, keepdims=True)

    def small_start(i, block):
        scs[i, 0] = block
        for k in range(1, NY):
            send(scs.at[i, 0], scr.at[i, k], sem_cs.at[i, 0], sem_cr.at[i, k], y=yp[k])

    def small_middle(i):
        sent(scr.at[i, pl.ds(0, NY - 1)], sem_cs.at[i, 0])
        total = scs[i, 0]
        for k in range(1, NY):
            arrived(scr.at[i, k], sem_cs.at[i, 0], sem_cr.at[i, k], y=yp[k])
            total = total + scr[i, k]
        scs[i, 1] = total
        for k in range(1, NZ):
            send(scs.at[i, 1], scr.at[i, NY + k], sem_cs.at[i, 1], sem_cr.at[i, NY + k], z=zp[k])

    def small_end(i):
        sent(scr.at[i, pl.ds(0, NZ - 1)], sem_cs.at[i, 1])
        total = scs[i, 1]
        for k in range(1, NZ):
            arrived(scr.at[i, NY + k], sem_cs.at[i, 1], sem_cr.at[i, NY + k], z=zp[k])
            total = total + scr[i, NY + k]
        return total

    half = NZ // 2 * RB

    def long_way(j):
        return 0 if j in (0, 3) else 1

    def along_z(way, links):
        return zp[links] if way == 0 else zm[links]

    def scatter(st, w, early, late, fill):
        ways_y = ((0, yp[1]), (1, ym[1]))

        def send_b(way, kind, peer):
            send(sb.at[st, way, kind], rb.at[st, way, kind], sem_sb.at[st], sem_rb.at[way, kind], y=peer)

        def got_b(way, kind):
            arrived(rb.at[st, way, kind], sem_sb.at[st], sem_rb.at[way, kind], y=yp[1])

        def send_a(way, s, j):
            send(
                sa.at[st, way, s, j], ra.at[st, way, s, j], sem_sa.at[st, way, abs(long_way(j) - way)],
                sem_ra.at[way, s, j], z=along_z(way, 2 if s == 0 else 1),
            )

        def got_a(way, s, j):
            arrived(ra.at[st, way, s, j], sem_sa.at[st, way, 0], sem_ra.at[way, s, j], z=zp[1])

        part = dot(at_b(yp[2]), w).reshape(2, NZ // 2, RB, 128)
        for way, peer in ways_y:
            sb[st, way, 0] = enc_b(part[way])
            send_b(way, 0, peer)
        far = enc_a(dot(at_a(zp[4]), w).reshape(NY, RA, 128))
        for j in range(NY):
            sa[st, long_way(j), 0, j] = far[j]
            send_a(long_way(j), 0, j)
        for way in range(2):
            sa[st, way, 1] = enc_a(dot(at_a(along_z(way, 3)), w).reshape(NY, RA, 128))
            for j in range(NY):
                send_a(way, 1, j)
        for way, peer in ways_y:
            part = dot(at_b(peer), w).reshape(2, NZ // 2, RB, 128)
            sb[st, way, 1] = enc_b(part[1 - way])
            send_b(way, 1, peer)
            y_c[way] = part[way]

        def product(i, carry):
            target = lax.rem(z + NZ - 2 + i, NZ)
            y_a[target] = dot(at_a(target), w).reshape(NY, RA, 128)
            return carry

        lax.fori_loop(0, 5, product, 0)
        y_b[...] = dot(at_b(y), w).reshape(NZ, RB, 128)
        early()
        for i in range(2):
            fill(i)

        def pass_on(s, j):
            codes = []
            for way in range(2):
                got_a(way, s - 1, j)
                if s == 2 and way == long_way(j):
                    got_a(way, 0, j)
            for way in range(2):
                total = dec_a(ra[st, way, s - 1, j]) + y_a[along_z(way, 4 - s), j]
                if s == 2 and way == long_way(j):
                    total = total + dec_a(ra[st, way, 0, j])
                codes.append(enc_a(total))
            for way in range(2):
                sa[st, way, s, j] = codes[way]
            for way in range(2):
                send_a(way, s, j)

        pass_on(2, 0)
        pass_on(2, 1)
        for way, peer in ways_y:
            got_b(way, 0)
            sb[st, way, 2] = enc_b(y_c[way] + dec_b(rb[st, way, 0]))
            send_b(way, 2, peer)
        pass_on(2, 2)
        pass_on(2, 3)
        fill(2)
        for j in range(NY):
            pass_on(3, j)
        late()
        for i in range(3, 6):
            fill(i)
        for way in range(2):
            for kind in (1, 2):
                got_b(way, kind)
        low = y_b[0 : NZ // 2] + dec_b(rb[st, 0, 2]) + dec_b(rb[st, 1, 1])
        y_b[0 : NZ // 2] = low
        szb[st, 0 : NZ // 2] = enc_b(low)
        high = y_b[NZ // 2 :] + dec_b(rb[st, 0, 1]) + dec_b(rb[st, 1, 2])
        y_b[NZ // 2 :] = high
        szb[st, NZ // 2 :] = enc_b(high)
        for k in (4, 3, 5, 2, 6, 1, 7):
            send(szb.at[st, zp[k]], rzb.at[st, k], sem_szb.at[st], sem_rzb.at[k], z=zp[k])
        for j in range(NY):
            for way in range(2):
                got_a(way, 3, j)
            total = dec_a(ra[st, 0, 3, j]) + dec_a(ra[st, 1, 3, j]) + y_a[z, j]
            y_a[z, j] = total
            sya[st, j] = enc_a(total)
        for k in (2, 1, 3):
            send(sya.at[st, yp[k]], rya.at[st, k], sem_sya.at[st], sem_rya.at[k], y=yp[k])
        for i in range(6, 11):
            fill(i)
        sum_b = y_b[z]
        for k in (1, 7, 2, 6, 3, 5, 4):
            arrived(rzb.at[st, k], sem_szb.at[st], sem_rzb.at[k], z=zp[k])
            sum_b = sum_b + dec_b(rzb[st, k])
        sum_a = y_a[z, y]
        for k in (1, 3, 2):
            arrived(rya.at[st, k], sem_sya.at[st], sem_rya.at[k], y=yp[k])
            sum_a = sum_a + dec_a(rya[st, k])
        for way in range(2):
            sent(sa.at[st, way, :, pl.ds(0, 2)], sem_sa.at[st, way, 0])
            sent(sa.at[st, way, pl.ds(0, 3), pl.ds(0, 2)], sem_sa.at[st, way, 1])
        sent(sb.at[st], sem_sb.at[st])
        sent(szb.at[st, pl.ds(0, NZ - 1)], sem_szb.at[st])
        sent(sya.at[st, pl.ds(0, NY - 1)], sem_sya.at[st])
        return sum_a, sum_b

    first_half, second_half = (0, 1, 7, 2), (6, 3, 5, 4)

    def gathered_product(it, rows_a, rows_b, middle):
        ga[it, z, y, 0:RA] = rows_a.astype(BF16)
        gb[it, y, z, 0:RB] = rows_b.astype(BF16)

        def part_a(it, zz, yy):
            return ga.at[it, zz, yy, pl.ds(0, RA)]

        def part_b(it, yy, zz):
            return gb.at[it, yy, zz, pl.ds(0, RB)]

        def put_a(way, s, k):
            block = part_a(it, along_z(1 - way, s - 1 if s else 2), ym[k])
            send(block, block, sem_gs.at[it, 0], sem_ga.at[way, s, k], z=along_z(way, 1 if s else 2))

        def got_a(way, s, k):
            block = part_a(it, along_z(1 - way, s if s else 4), ym[k])
            arrived(block, sem_gs.at[it, 0], sem_ga.at[way, s, k], z=zp[1])

        def put_b(way, s, k):
            block = part_b(it, ym[s] if way == 0 else yp[s], zm[k])
            send(block, block, sem_gs.at[it, 1], sem_gby.at[way, s, k], y=yp[1] if way == 0 else ym[1])

        def got_b(way, s, k):
            block = part_b(it, ym[s + 1] if way == 0 else yp[s + 1], zm[k])
            arrived(block, sem_gs.at[it, 1], sem_gby.at[way, s, k], y=yp[1])

        def from_z(k):
            arrived(part_b(it, y, zm[k]), sem_gs.at[it, 3], sem_gb.at[k], z=zp[k])
            if k == 5:
                send(part_b(it, y, zm[5]), part_b(it, y, zm[5]), sem_gs.at[it, 3], sem_gb.at[4], z=zm[1])
            put_b(0, 0, k)
            put_b(1, 0, k)

        own_a, own_b = part_a(it, z, y), part_b(it, y, z)
        for k in (2, 1, 3):
            send(own_a, own_a, sem_gs.at[it, 2], sem_gay.at[k], y=yp[k])
        put_a(0, 1, 0)
        put_a(1, 1, 0)
        for k in (5, 3, 2, 6, 1, 7):
            send(own_b, own_b, sem_gs.at[it, 3], sem_gb.at[k], z=zp[k])
        put_b(0, 0, 0)
        put_b(1, 0, 0)
        def pass_a(s, blocks):
            for k in blocks:
                for way in range(2):
                    got_a(way, s, k)
                    if s == 2 and way == long_way(k):
                        put_a(way, 0, k)
                    if s < 3:
                        put_a(way, s + 1, k)

        def pass_b(blocks):
            for k in blocks:
                way = 0 if k in first_half else 1
                got_b(way, 0, k)
                put_b(way, 1, k)

        def times_a(v, zz):
            return v + dot(aa[zz], ga[it, zz].reshape(NY * LANES, LANES))

        def times_b(v, yy):
            return v + dot(ab[yy], gb[it, yy].reshape(NZ * LANES, LANES))

        for k in (1, 3, 2):
            arrived(part_a(it, z, ym[k]), sem_gs.at[it, 2], sem_gay.at[k], y=yp[k])
            put_a(0, 1, k)
            put_a(1, 1, k)
        pass_a(1, (0,))
        pass_b((0,))
        for k in (1, 7, 2, 6):
            from_z(k)
        middle()
        for k in (5, 3):
            from_z(k)
        v = dot(aa[z], ga[it, z].reshape(NY * LANES, LANES))
        pass_a(1, (1, 3, 2))
        pass_a(2, (0,))
        pass_b((1, 7, 2, 6))
        v = times_a(times_a(v, zm[1]), zp[1])
        pass_b((5, 3))
        from_z(4)
        pass_a(2, (1, 3, 2))
        pass_a(3, (0,))
        v = times_b(times_a(times_a(v, zm[2]), zp[2]), y)
        pass_b((4,))
        for k in second_half:
            got_b(0, 0, k)
        for k in first_half:
            got_b(1, 0, k)
        v = times_b(times_b(v, yp[1]), ym[1])
        pass_a(3, (1, 3, 2))
        v = times_a(times_a(v, zm[3]), zp[3])
        for k in first_half:
            got_b(0, 1, k)
        for k in second_half:
            got_b(1, 1, k)
        v = times_b(v, yp[2])
        for k in range(NY):
            got_a(long_way(k), 0, k)
        sent(ga.at[it, pl.ds(0, NZ - 1), :, pl.ds(0, RA)], sem_gs.at[it, 0])
        sent(gb.at[it, pl.ds(0, NY - 1), :, pl.ds(0, RB)], sem_gs.at[it, 1])
        sent(ga.at[it, 0, pl.ds(0, NY - 1), pl.ds(0, RA)], sem_gs.at[it, 2])
        sent(gb.at[it, 0, pl.ds(0, NZ - 1), pl.ds(0, RB)], sem_gs.at[it, 3])
        return v + dot(aa[zm[4]], ga[it, zm[4]].reshape(NY * LANES, LANES))

    def slab_values(it, v, scal, finish):
        vs[it] = v.reshape(2, BAND, 128)
        scc[it, 0] = scal
        send(vs.at[it, other], vr.at[it], sem_vs.at[it, 0], sem_vr.at[it, 0], c=other)
        send(scc.at[it, 0], scc.at[it, 1], sem_vs.at[it, 1], sem_vr.at[it, 1], c=other)
        arrived(vr.at[it], sem_vs.at[it, 0], sem_vr.at[it, 0], c=other)
        chip = vs[it, c] + vr[it]
        us[it] = enc_v(chip)
        for k in (2, 1, 3):
            send(us.at[it], ur.at[it, k], sem_us.at[it, 0], sem_ur.at[it, k], x=xp[k])
        arrived(scc.at[it, 1], sem_vs.at[it, 1], sem_vr.at[it, 1], c=other)
        scal = scc[it, 0] + scc[it, 1]
        scx[it, 0] = scal
        for k in (2, 1, 3):
            send(scx.at[it, 0], scx.at[it, k], sem_us.at[it, 1], sem_uc.at[it, k], x=xp[k])
        for k in (1, 3, 2):
            arrived(ur.at[it, k], sem_us.at[it, 0], sem_ur.at[it, k], x=xp[k])
            chip = chip + dec_v(ur[it, k])
            arrived(scx.at[it, k], sem_us.at[it, 1], sem_uc.at[it, k], x=xp[k])
            scal = scal + scx[it, k]
        mask = wm[pl.ds(pl.multiple_of(c * BAND, BAND), BAND), :]
        block, scal = finish(mask * chip, scal)
        hq[it + 1, 1 + c] = enc_v(block)
        slot = 3 - 3 * c
        step = jnp.where(c == 0, t_down, t_up)
        mine = hq.at[it + 1, 1 + c]
        for core in range(NC):
            send(
                mine, hq.at[it + 1, slot], sem_hs.at[it + 1, 1 + core], sem_hr.at[it + 1, slot],
                z=lax.div(step, NY), y=lax.rem(step, NY), c=jnp.int32(core),
            )
        send(mine, mine, sem_hs.at[it + 1, 0], sem_hr.at[it + 1, 1 + c], c=other)
        for k in range(3):
            sent(mine, sem_hs.at[it + 1, k])
        sent(vs.at[it, 0], sem_vs.at[it, 0])
        sent(scc.at[it, 0], sem_vs.at[it, 1])
        sent(ur.at[it, pl.ds(0, NX - 1)], sem_us.at[it, 0])
        sent(scx.at[it, pl.ds(0, NX - 1)], sem_us.at[it, 1])
        for place in (2 - c, 0, 3):
            arrived(hq.at[it + 1, place], sem_hs.at[it + 1, 0], sem_hr.at[it + 1, place], c=other)
        return block, scal

    arrived(hq.at[0, 0], sem_hs.at[0, 0], sem_hr.at[0, 0], c=other)
    arrived(hq.at[0, 3], sem_hs.at[0, 0], sem_hr.at[0, 3], c=other)

    def nothing(*_):
        return None

    def some_columns(i):
        lax.fori_loop(3 * i, min(3 * i + 3, NZ * NY), put_columns, 0)

    w, _ = filtered(0)
    res_a, res_b = scatter(0, w, nothing, nothing, some_columns)

    def col_sum(a, b):
        return jnp.sum(a, 0, keepdims=True) + jnp.sum(b, 0, keepdims=True)

    def rows_of(*rows):
        spare = jnp.zeros((8 - len(rows), 128), F32)
        return jnp.concatenate([*rows, spare], 0)

    dir_a, dir_b = pca[...] * res_a, pcb[...] * res_b
    small_start(0, rows_of(col_sum(res_a * dir_a, res_b * dir_b), col_sum(kda[...] * dir_a * dir_a, kdb[...] * dir_b * dir_b)))
    v = gathered_product(0, dir_a, dir_b, lambda: small_middle(0))
    block, scal = slab_values(0, v, small_end(0), lambda block, scal: (block, scal))
    norm, diag = scal[0:1], scal[1:2]

    w, inner = filtered(1)
    image_a, image_b = scatter(1, w, lambda: small_start(1, rows_of(inner)), lambda: small_middle(1), nothing)
    step_len = norm / (diag + small_end(1)[0:1])
    image_a, image_b = image_a + kda[...] * dir_a, image_b + kdb[...] * dir_b
    sol_a, sol_b = step_len * dir_a, step_len * dir_b
    res_a, res_b = res_a - step_len * image_a, res_b - step_len * image_b
    scaled_a, scaled_b = pca[...] * res_a, pcb[...] * res_b
    small_start(
        2,
        rows_of(
            col_sum(res_a * scaled_a, res_b * scaled_b),
            col_sum(kda[...] * scaled_a * scaled_a, kdb[...] * scaled_b * scaled_b),
            col_sum(kda[...] * scaled_a * dir_a, kdb[...] * scaled_b * dir_b),
        ),
    )
    v = gathered_product(1, scaled_a, scaled_b, lambda: small_middle(2))

    def finish(new_block, scal):
        ratio = scal[0:1] / norm
        return new_block + ratio * block, scal

    _, scal = slab_values(1, v, small_end(2), finish)
    ratio = scal[0:1] / norm
    norm = scal[0:1]
    diag = scal[1:2] + 2.0 * ratio * scal[2:3] + ratio * ratio * diag
    dir_a, dir_b = scaled_a + ratio * dir_a, scaled_b + ratio * dir_b
    w, last_inner = filtered(2)
    image_a, image_b = scatter(2, w, lambda: small_start(3, rows_of(last_inner)), lambda: small_middle(3), nothing)
    step_len = norm / (diag + small_end(3)[0:1])
    image_a, image_b = image_a + kda[...] * dir_a, image_b + kdb[...] * dir_b
    sol_a, sol_b = sol_a + step_len * dir_a, sol_b + step_len * dir_b
    res_a, res_b = res_a - step_len * image_a, res_b - step_len * image_b
    xout[0:NA] = sol_a[0:NA]
    xout[NA:] = sol_b[0:NB]
    rout[0:NA] = res_a[0:NA]
    rout[NA:] = res_b[0:NB]
    for copy in pending:
        copy.wait_send()


def shards(design, observed, slab_counts, gap_mask, filter_taps, kaula_diag, precond):
    rows = observed.shape[0]
    coefs = design.shape[1]
    dma = pltpu.SemaphoreType.DMA
    args = (
        design, observed, slab_counts, gap_mask.reshape(rows // LANES, LANES), filter_taps.reshape(1, LANES),
        kaula_diag.reshape(coefs // LANES, LANES), precond.reshape(coefs // LANES, LANES),
    )
    vm = pltpu.VMEM
    scratch = [
        vm((NZ, rows, NY * LANES), BF16),
        vm((NY, rows, NZ * LANES), BF16),
        vm((NZ, NY, RA, rows), BF16),
        vm((NY, NZ, RB, rows), BF16),
        vm((rows, LANES), F32),
        vm((RA, LANES), F32), vm((RB, LANES), F32), vm((RA, LANES), F32), vm((RB, LANES), F32),
        vm((4 * LANES, LANES), F32),
        vm((2 * BAND, 4 * BAND), F32), vm((2 * BAND, 4 * BAND), BF16), vm((2 * BAND, 4 * BAND), BF16),
        vm((NZ, NY, RA, 128), F32),
        vm((NZ, RB, 128), F32),
        vm((2, NZ // 2, RB, 128), F32),
        vm((3, 2, 4, NY, RA, 128), I16),
        vm((3, 2, 4, NY, RA, 128), I16),
        vm((3, NY, RA, 128), I16),
        vm((3, NY, RA, 128), I16),
        vm((3, 2, 3, NZ // 2, RB, 128), I16),
        vm((3, 2, 3, NZ // 2, RB, 128), I16),
        vm((3, NZ, RB, 128), I16),
        vm((3, NZ, RB, 128), I16),
        vm((2, NZ, NY, LANES, LANES), BF16),
        vm((2, NY, NZ, LANES, LANES), BF16),
        vm((2, 2, BAND, 128), F32),
        vm((2, BAND, 128), F32),
        vm((2, BAND + 16, 128), I16),
        vm((2, NX, BAND + 16, 128), I16),
        vm((3, 4, BAND + 16, 128), I16),
        vm((4, 2, 8, 128), F32),
        vm((4, NY + NZ, 8, 128), F32),
        vm((2, 2, 8, 128), F32),
        vm((2, NX, 8, 128), F32),
        dma((3, 2, 2)), dma((2, 4, NY)), dma((3,)), dma((NY,)),
        dma((3,)), dma((2, 3)), dma((3,)), dma((NZ,)),
        dma((2, 4)), dma((2, 4, NY)), dma((NY,)), dma((NZ,)), dma((2, 2, NZ)),
        dma((2, 2)), dma((2, 2)), dma((2, 2)), dma((2, NX)), dma((2, NX)), dma((3, 4)), dma((3, 4)),
        dma((4, 2)), dma((4, NY + NZ)),
    ]
    out = jax.ShapeDtypeStruct((OWN, LANES), F32)
    return pl.pallas_call(
        kernel,
        name="cg",
        out_shape=(out, out),
        in_specs=[pl.BlockSpec(memory_space=pltpu.SMEM if i == 2 else vm) for i in range(len(args))],
        out_specs=(pl.BlockSpec(memory_space=vm),) * 2,
        scratch_shapes=scratch,
        compiler_params=pltpu.CompilerParams(
            collective_id=0, has_side_effects=True, vmem_limit_bytes=60 * 1024 * 1024
        ),
    )(*args)


def solution(mesh):
    torus = Mesh(mesh.devices.reshape(NZ, NY, NX, NC), AXES)
    in_specs = (P(TM, COEF), P(TM, None), P(TM), P(TM), P(), P(COEF), P(COEF))
    out_specs = (P((*COEF, *TM), None),) * 2
    return jax.shard_map(shards, mesh=torus, in_specs=in_specs, out_specs=out_specs, check_vma=False)
```
